256 devices in a mesh: gx: 16 (over z_lo, x), gy: 4 (over y), gz: 4 (over z_hi, core).
Axes of the slice: x: 4, y: 4, z: 8 (z_hi: 2, z_lo: 4; z = z_hi * 4 + z_lo), core: 2. Of those that a mesh axis runs over, the one named last changes fastest.
Arguments:
- tokens: bfloat16 [8192, 4608], P('gx', 'gy'), may hold values from -6 to 6
- base_up_weight: bfloat16 [4608, 18432], P('gy', ('gz', 'gx')), may hold values from -0.09375 to 0.09375
- adapter_down_weight: bfloat16 [64, 16, 4608], P(None, None, 'gy'), may hold values from -0.09375 to 0.09375
- adapter_up_weight: bfloat16 [64, 16, 18432], P('gx', None, 'gz'), may hold values from -1.5 to 1.5
- block_adapter_index: int32 [64], P('gx'), may hold values from 0 to 63
- request_rows: int32 [64], P('gx'), may hold values from 1 to 128
Outputs:
- projected: bfloat16 [8192, 18432], P(('gx', 'gy'), 'gz')
The draws below stay inside these ranges and needn't reach their ends.
Inputs may be any that keep to these rules, and one draw needn't show every extreme that they name: `request_rows`: live rows of each block.
All inputs are finite; a program needn't handle non-finite values.
Results may differ from the reference program's by a relative error of at most 0.0047.
Values may be sent and summed in bfloat16 or wider, within the bound.
No kernel may reach another device: no remote copies, remote signals or barrier semaphores. Data moves between devices by JAX's collectives and lax.ppermute only.
A program may use at most 128 MiB of HBM per device.

```python
import jax
import jax.numpy as jnp
from jax import lax

MODEL_WIDTH = 4608
HIDDEN_UNITS = 18432
ADAPTER_RANK = 16
ADAPTER_COUNT = 64
BLOCK = 128
BLOCKS = 64
ROWS = 8192


def touch_ends(array, rng, low, largest):
    place = [jax.random.randint(jax.random.fold_in(rng, axis), (), 0, length) for axis, length in enumerate(array.shape)]
    main_axis = array.shape.index(max(array.shape))
    beside = place[:main_axis] + [(place[main_axis] + 1) % array.shape[main_axis]] + place[main_axis + 1:]
    return array.at[tuple(place)].set(low).at[tuple(beside)].set(largest)


def block_scale(own_key, shape, pieces, least, high):
    factor_of = 1.0
    for axis_at, parts in pieces:
        steps = jax.random.uniform(jax.random.fold_in(jax.random.fold_in(own_key, 6), axis_at), (parts,), jnp.float32, least / len(pieces), high / len(pieces))
        factor_of = factor_of * jnp.repeat(jnp.exp(steps), shape[axis_at] // parts).reshape((-1,) + (1,) * (len(shape) - 1 - axis_at))
    return factor_of


def gaussian(key, dims, scale, most, shards=(), kind=jnp.bfloat16):
    values = scale * jax.random.normal(key, dims, jnp.float32)
    if shards:
        values = values * block_scale(key, dims, shards, -0.22, 0.18)
    return jnp.clip(values, -most, most).astype(kind)


def setup_inputs(seed: int = 0) -> dict:
    streams_of = jax.random.split(jax.random.key(seed), 7)
    return {
        "tokens": gaussian(streams_of[0], (ROWS, MODEL_WIDTH), 1.0, 6.0, ((0, 16), (1, 4))),
        "base_up_weight": gaussian(streams_of[1], (MODEL_WIDTH, HIDDEN_UNITS), MODEL_WIDTH ** -0.5, 0.09375, ((0, 4), (1, 64))),
        "adapter_down_weight": gaussian(streams_of[2], (ADAPTER_COUNT, ADAPTER_RANK, MODEL_WIDTH), MODEL_WIDTH ** -0.5, 0.09375, ((2, 4),)),
        "adapter_up_weight": gaussian(streams_of[3], (ADAPTER_COUNT, ADAPTER_RANK, HIDDEN_UNITS), ADAPTER_RANK ** -0.5, 1.5, ((0, 16), (2, 4))),
        "block_adapter_index": touch_ends(jax.random.randint(streams_of[4], (BLOCKS,), 0, ADAPTER_COUNT), jax.random.fold_in(streams_of[4], 1), 0, ADAPTER_COUNT - 1).astype(jnp.int32),
        "request_rows": touch_ends(jax.random.randint(streams_of[5], (BLOCKS,), 1, BLOCK + 1), jax.random.fold_in(streams_of[5], 1), 1, BLOCK).astype(jnp.int32),
    }


def reference(tokens, base_up_weight, adapter_down_weight, adapter_up_weight, block_adapter_index, request_rows):
    blocks = block_adapter_index.shape[0]
    tok_blocks = tokens.reshape(blocks, BLOCK, MODEL_WIDTH)

    def one_block(items):
        block_tokens, adapter_index, live_count = items
        down_factor = lax.dynamic_index_in_dim(adapter_down_weight, adapter_index, 0, keepdims=False)
        up_factor = lax.dynamic_index_in_dim(adapter_up_weight, adapter_index, 0, keepdims=False)
        shrink = jnp.dot(block_tokens, down_factor.T, preferred_element_type=jnp.float32)
        shrink_low = shrink.astype(jnp.bfloat16)
        expand = jnp.dot(shrink_low, up_factor, preferred_element_type=jnp.float32)
        base = jnp.dot(block_tokens, base_up_weight, preferred_element_type=jnp.float32)
        live_mask = jnp.arange(BLOCK, dtype=jnp.int32) < live_count
        return jnp.where(live_mask[:, None], base + 2.0 * expand, 0.0).astype(jnp.bfloat16)

    result = lax.map(one_block, (tok_blocks, block_adapter_index, request_rows))
    return result.reshape(blocks * BLOCK, HIDDEN_UNITS)
```

```python
import jax
import jax.numpy as jnp
from jax import lax
from jax.experimental import pallas as pl
from jax.experimental.pallas import tpu as pltpu
from jax.sharding import PartitionSpec as P

BLOCK = 128
ZL, NX, NY, ZH, NC = 4, 4, 4, 2, 2


def x_perm(shift):
    return [(z * NX + x, z * NX + (x + shift) % NX) for z in range(ZL) for x in range(NX)]


def zl_perm(shift):
    return [(z * NX + x, (z + shift) % ZL * NX + x) for z in range(ZL) for x in range(NX)]


def ring_perm(shift):
    pairs = []
    for z in range(ZL * ZH):
        t = (z + shift) % (ZL * ZH)
        for x in range(NX):
            for c in range(NC):
                src = (z % ZL * NX + x) * ZH * NC + z // ZL * NC + c
                dst = (t % ZL * NX + x) * ZH * NC + t // ZL * NC + c
                pairs.append((src, dst))
    return pairs


def along_x(a, shift):
    return lax.ppermute(a, "gx", x_perm(shift))


def along_zl(a, shift):
    return lax.ppermute(a, "gx", zl_perm(shift))


def along_z(a, shift):
    return lax.ppermute(a, ("gx", "gz"), ring_perm(shift))


def along_y(a, shift):
    return lax.ppermute(a, "gy", [(y, (y + shift) % NY) for y in range(NY)])


def across_cores(a):
    return lax.ppermute(a, "gz", [(g, g ^ 1) for g in range(ZH * NC)])


def nt_dot(a, b):
    return lax.dot_general(a, b, (((1,), (1,)), ((), ())), preferred_element_type=jnp.float32)


def vmem():
    return pl.BlockSpec(memory_space=pltpu.VMEM)


def smem():
    return pl.BlockSpec(memory_space=pltpu.SMEM)


def shrink_kernel(index_ref, tok_ref, down_ref, out_ref):
    out_ref[0] = nt_dot(down_ref[0], tok_ref[...])


def shrink(tokens, down, index):
    rows, width = tokens.shape
    blocks = rows // BLOCK
    rank = down.shape[1]
    spec = pltpu.PrefetchScalarGridSpec(
        num_scalar_prefetch=1,
        grid=(blocks,),
        in_specs=[
            pl.BlockSpec((BLOCK, width), lambda b, idx: (b, 0)),
            pl.BlockSpec((1, rank, width), lambda b, idx: (idx[b], 0, 0)),
        ],
        out_specs=pl.BlockSpec((1, rank, BLOCK), lambda b, idx: (b, 0, 0)),
    )
    return pl.pallas_call(
        shrink_kernel,
        grid_spec=spec,
        out_shape=jax.ShapeDtypeStruct((blocks, rank, BLOCK), jnp.float32),
        name="shrink",
    )(index, tokens, down)


def partial_kernel(place_ref, *refs):
    lhs, w_ref, outs = refs[:-5], refs[-5], refs[-4:]
    blocks = []
    for ref in lhs:
        for j in range(ref.shape[0] // BLOCK):
            blocks.append((ref, j))
    for i, (ref, j) in enumerate(blocks):
        value = nt_dot(ref[pl.ds(j * BLOCK, BLOCK), :], w_ref[...]).astype(jnp.bfloat16)
        for k in range(NY):
            @pl.when(place_ref[i] == k)
            def _():
                outs[k][...] = value


def partial_products(place, lhs, w_all):
    n = w_all.shape[0]
    shape = jax.ShapeDtypeStruct((BLOCK, n), jnp.bfloat16)
    rows = sum(a.shape[0] for a in lhs)
    width = w_all.shape[1]
    return pl.pallas_call(
        partial_kernel,
        in_specs=[smem()] + [vmem()] * (len(lhs) + 1),
        out_specs=[vmem()] * NY,
        out_shape=[shape] * NY,
        cost_estimate=pl.CostEstimate(
            flops=2 * rows * width * n, bytes_accessed=2 * (rows * width + width * n + rows * n), transcendentals=0
        ),
        name="partial_products",
    )(place, *lhs, w_all)


def finish_kernel(col_ref, live_ref, shrink_ref, up_ref, *refs):
    pieces, out_ref = refs[:-1], refs[-1]
    n = pieces[0].shape[1]
    low = shrink_ref[...]
    mask = lax.broadcasted_iota(jnp.int32, (BLOCK, n), 0) < live_ref[0]
    for r, piece in enumerate(pieces):
        at = pl.multiple_of(col_ref[r] * n, 128)
        expand = lax.dot_general(
            low, up_ref[col_ref[r]], (((0,), (0,)), ((), ())), preferred_element_type=jnp.float32
        )
        total = piece[...].astype(jnp.float32) + 2.0 * expand
        out_ref[:, pl.ds(at, n)] = jnp.where(mask, total, 0.0).astype(jnp.bfloat16)


def finish(cols, live, low, up, pieces):
    n = pieces[0].shape[1]
    return pl.pallas_call(
        finish_kernel,
        in_specs=[smem(), smem()] + [vmem()] * (2 + len(pieces)),
        out_specs=vmem(),
        out_shape=jax.ShapeDtypeStruct((BLOCK, n * len(pieces)), jnp.bfloat16),
        name="finish",
    )(cols, live, low, up, *pieces)


def reduced_over_y(parts):
    own, plus, far, minus = parts
    half = BLOCK // 2
    up = along_y(far[:half], 1)
    down = along_y(far[half:], -1)
    f32 = jnp.float32
    to_plus = jnp.concatenate(
        [(plus[:half].astype(f32) + up.astype(f32)).astype(jnp.bfloat16), plus[half:]], axis=0
    )
    to_minus = jnp.concatenate(
        [minus[:half], (minus[half:].astype(f32) + down.astype(f32)).astype(jnp.bfloat16)], axis=0
    )
    a = along_y(to_plus, 1)
    b = along_y(to_minus, -1)
    return (own.astype(f32) + a.astype(f32) + b.astype(f32)).astype(jnp.bfloat16)


def body(tokens, base_up_weight, adapter_down_weight, adapter_up_weight, block_adapter_index, request_rows):
    rows, width = tokens.shape
    x = lax.axis_index("gx") % NX
    zl = lax.axis_index("gx") // NX
    y = lax.axis_index("gy")
    c = lax.axis_index("gz") % NC
    half = rows // NC
    quarter = half // 2

    mine = lax.dynamic_slice_in_dim(tokens, c * half, half, 0)
    w_own = base_up_weight.T
    from_left = along_z(mine, 1)
    from_right = along_z(mine, -1)
    w_left = along_x(w_own, 1)
    w_right = along_x(w_own, -1)
    far_a = along_z(from_left[:quarter], 1)
    far_b = along_z(from_right[quarter:], -1)
    nb = w_own.shape[0]
    w_far_a = along_x(w_left[: nb // 2], 1)
    w_far_b = along_x(w_right[nb // 2 :], -1)
    other_left = across_cores(from_left)
    other_right = across_cores(from_right)
    other_a = across_cores(far_a)
    other_b = across_cores(far_b)

    shrink_part = shrink(tokens, adapter_down_weight, block_adapter_index)
    shrink_all = lax.all_to_all(shrink_part, "gy", 0, 0, tiled=True)
    low = jnp.sum(shrink_all, axis=0).astype(jnp.bfloat16)

    w_all = jnp.zeros((NX, nb, width), jnp.bfloat16)
    w_all = lax.dynamic_update_slice(w_all, w_own[None], (x, 0, 0))
    w_all = lax.dynamic_update_slice(w_all, w_left[None], ((x + 3) % NX, 0, 0))
    w_all = lax.dynamic_update_slice(w_all, w_right[None], ((x + 1) % NX, 0, 0))
    w_all = lax.dynamic_update_slice(w_all, w_far_a[None], ((x + 2) % NX, 0, 0))
    w_all = lax.dynamic_update_slice(w_all, w_far_b[None], ((x + 2) % NX, nb // 2, 0))
    w_all = w_all.reshape(NX * nb, width)

    order = jnp.arange(NY, dtype=jnp.int32)
    own_place = (order - y) % NY
    shared_place = ((order // 2 ^ c) * 2 + order % 2 - y) % NY
    left = partial_products(shared_place, (from_left, other_left), w_all)
    right = partial_products(shared_place, (from_right, other_right), w_all)
    far = partial_products(shared_place, (far_a, far_b, other_a, other_b), w_all)
    own = partial_products(own_place, (tokens,), w_all)
    sum_left = reduced_over_y(left)
    sum_far = reduced_over_y(far)
    sum_right = reduced_over_y(right)
    sum_own = reduced_over_y(own)
    piece_left = along_zl(sum_left, -1)
    piece_right = along_zl(sum_right, 1)
    piece_far = along_zl(sum_far, 2)

    n = w_all.shape[0]
    up_own = lax.dynamic_slice_in_dim(adapter_up_weight, y * n, n, 2)
    up_z = [up_own, along_zl(up_own, 3), along_zl(up_own, 2), along_zl(up_own, 1)]
    up_z = jnp.stack(up_z)
    up_left = along_x(up_z, 1)
    up_right = along_x(up_z, -1)
    up_far_a = along_x(up_left[:2], 1)
    up_far_b = along_x(up_right[2:], -1)
    up_all = jnp.concatenate([up_z, up_right, up_far_a, up_far_b, up_left]).reshape(
        NX * ZL * up_own.shape[0], *up_own.shape[1:]
    )
    owner = block_adapter_index // up_own.shape[0]
    at = ((owner % NX - x) % NX * ZL + (owner // NX - zl) % ZL) * up_own.shape[0] + block_adapter_index % up_own.shape[0]
    picked = jnp.concatenate([lax.dynamic_slice_in_dim(up_all, at[b], 1, 0) for b in range(NY)])
    up = lax.all_to_all(picked, "gy", 0, 0, tiled=True)

    live = lax.dynamic_slice_in_dim(request_rows, y, 1, 0)
    cols = (zl + jnp.array([0, 1, 3, 2], jnp.int32)) % ZL
    return finish(cols, live, low, up, (sum_own, piece_left, piece_right, piece_far))


def solution(mesh):
    in_specs = (
        P("gx", "gy"),
        P("gy", ("gz", "gx")),
        P(None, None, "gy"),
        P("gx", None, "gz"),
        P("gx"),
        P("gx"),
    )
    out_specs = P(("gx", "gy"), "gz")
    return jax.shard_map(body, mesh=mesh, in_specs=in_specs, out_specs=out_specs, check_vma=False)
```

```python
import jax
import jax.numpy as jnp
from jax import lax
from jax.experimental import pallas as pl
from jax.experimental.pallas import tpu as pltpu
from jax.sharding import PartitionSpec as P

BLOCK = 128
ZL, NX, NY, ZH, NC = 4, 4, 4, 2, 2
NZ = ZL * ZH
VMEM_LIMIT = 48 * 2**20


def device_perm(move):
    def place(z, x, c):
        return (z % ZL * NX + x) * ZH * NC + z // ZL * NC + c

    return [(place(z, x, c), place(*move(z, x, c))) for z in range(NZ) for x in range(NX) for c in range(NC)]


def send(a, move):
    return lax.ppermute(a, ("gx", "gz"), device_perm(move))


def within(z, shift):
    return z // ZL * ZL + (z + shift) % ZL


def along_x(a, shift):
    return lax.ppermute(a, "gx", [(z * NX + x, z * NX + (x + shift) % NX) for z in range(ZL) for x in range(NX)])


def along_y(a, shift):
    return lax.ppermute(a, "gy", [(y, (y + shift) % NY) for y in range(NY)])


def swap_cores(a):
    return send(a, lambda z, x, c: (z, x, 1 - c))


def nt_dot(a, b):
    return lax.dot_general(a, b, (((1,), (1,)), ((), ())), preferred_element_type=jnp.float32)


def hbm():
    return pl.BlockSpec(memory_space=pltpu.HBM)


def smem():
    return pl.BlockSpec(memory_space=pltpu.SMEM)


def params():
    return pltpu.CompilerParams(vmem_limit_bytes=VMEM_LIMIT)


def shrink_kernel(index_ref, tok_ref, down_ref, out_ref):
    out_ref[0] = nt_dot(down_ref[0], tok_ref[...])


def shrink(tokens, down, index):
    rows, width = tokens.shape
    blocks = rows // BLOCK
    rank = down.shape[1]
    spec = pltpu.PrefetchScalarGridSpec(
        num_scalar_prefetch=1,
        grid=(blocks,),
        in_specs=[
            pl.BlockSpec((BLOCK, width), lambda b, idx: (b, 0)),
            pl.BlockSpec((1, rank, width), lambda b, idx: (idx[b], 0, 0)),
        ],
        out_specs=pl.BlockSpec((1, rank, BLOCK), lambda b, idx: (b, 0, 0)),
    )
    return pl.pallas_call(
        shrink_kernel,
        grid_spec=spec,
        out_shape=jax.ShapeDtypeStruct((blocks, rank, BLOCK), jnp.float32),
        name="shrink",
    )(index, tokens, down)


def partial_products(chunks, weights):
    nb, width = weights[0].shape
    n = NX * nb
    count = len(chunks)
    rows = NY * BLOCK
    flat = [a for chunk in chunks for a in chunk]
    sizes = [len(chunk) for chunk in chunks]
    half = BLOCK // 2

    def kernel(*refs):
        ins, w_in = refs[: len(flat)], refs[len(flat) : len(flat) + NX]
        outs = refs[len(flat) + NX : len(flat) + NX + 5]
        t_ref, w_ref, o_ref, in_sems, w_sems, out_sems = refs[len(flat) + NX + 5 :]
        x = lax.axis_index("gx") % NX
        y = lax.axis_index("gy")
        c = lax.axis_index("gz") % NC
        w_copies = [
            pltpu.make_async_copy(
                w_in[r], w_ref.at[pl.ds(pl.multiple_of((x + r) % NX * nb, 16), nb), :], w_sems.at[r]
            )
            for r in range(NX)
        ]
        t_copies, at = [], 0
        for i, size in enumerate(sizes):
            part = rows // size
            copies = []
            for j in range(size):
                start = i * rows + (j if size == 1 else (c + j) % NC) * part
                copies.append(
                    pltpu.make_async_copy(
                        ins[at], t_ref.at[pl.ds(pl.multiple_of(start, BLOCK), part), :], in_sems.at[at]
                    )
                )
                at += 1
            t_copies.append(copies)
        for copy in t_copies[0] + w_copies:
            copy.start()
        for copies in t_copies[1:]:
            for copy in copies:
                copy.start()
        for copy in w_copies:
            copy.wait()
        done = []
        for i in range(count):
            for copy in t_copies[i]:
                copy.wait()
            o_ref[pl.ds(i * rows, rows), :] = nt_dot(
                t_ref[pl.ds(i * rows, rows), :], w_ref[...]
            ).astype(jnp.bfloat16)

            def rows_of(shift, low, size):
                start = i * rows + (y + shift) % NY * BLOCK + low
                return o_ref.at[pl.ds(pl.multiple_of(start, half), size), :]

            moves = [
                (rows_of(2, 0, half), outs[1].at[pl.ds(i * BLOCK, half), :]),
                (rows_of(1, half, half), outs[1].at[pl.ds(i * BLOCK + half, half), :]),
                (rows_of(3, 0, half), outs[2].at[pl.ds(i * BLOCK, half), :]),
                (rows_of(2, half, half), outs[2].at[pl.ds(i * BLOCK + half, half), :]),
                (rows_of(1, 0, half), outs[3].at[pl.ds(i * half, half), :]),
                (rows_of(3, half, half), outs[4].at[pl.ds(i * half, half), :]),
                (rows_of(0, 0, BLOCK), outs[0].at[pl.ds(i * BLOCK, BLOCK), :]),
            ]
            for k, (src, dst) in enumerate(moves):
                copy = pltpu.make_async_copy(src, dst, out_sems.at[i, k])
                copy.start()
                done.append(copy)
        for copy in done:
            copy.wait()

    def out(m):
        return jax.ShapeDtypeStruct((m * count, n), jnp.bfloat16)

    return pl.pallas_call(
        kernel,
        in_specs=[hbm()] * (len(flat) + NX),
        out_specs=[hbm()] * 5,
        out_shape=[out(BLOCK)] * 3 + [out(half)] * 2,
        scratch_shapes=[
            pltpu.VMEM((count * rows, width), jnp.bfloat16),
            pltpu.VMEM((n, width), jnp.bfloat16),
            pltpu.VMEM((count * rows, n), jnp.bfloat16),
            pltpu.SemaphoreType.DMA((len(flat),)),
            pltpu.SemaphoreType.DMA((NX,)),
            pltpu.SemaphoreType.DMA((count, 7)),
        ],
        cost_estimate=pl.CostEstimate(
            flops=2 * count * rows * width * n,
            bytes_accessed=2 * (count * rows * width + width * n + count * rows * n),
            transcendentals=0,
        ),
        compiler_params=params(),
        name="partial_products",
    )(*flat, *weights)


def wide(a):
    return a.astype(jnp.float32)


def step_one(parts):
    own, plus, minus, _, _ = parts
    return along_y(plus, 1), along_y(minus, -1)


def step_two(parts, first):
    half = BLOCK // 2
    own, _, _, plus, minus = parts
    count, n = own.shape[0] // BLOCK, own.shape[1]
    from_minus, from_plus = (a.reshape(count, 2, half, n) for a in first)
    plus, minus = plus.reshape(count, half, n), minus.reshape(count, half, n)
    a = along_y((wide(plus) + wide(from_minus[:, 0])).astype(jnp.bfloat16), 1)
    b = along_y((wide(minus) + wide(from_plus[:, 1])).astype(jnp.bfloat16), -1)
    return a, b


def summed(parts, first, second):
    half = BLOCK // 2
    own = parts[0]
    count, n = own.shape[0] // BLOCK, own.shape[1]
    from_minus, from_plus = (a.reshape(count, 2, half, n) for a in first)
    own = own.reshape(count, 2, half, n)
    low = wide(own[:, 0]) + wide(from_plus[:, 0]) + wide(second[0])
    high = wide(own[:, 1]) + wide(from_minus[:, 1]) + wide(second[1])
    return [jnp.concatenate([low[i], high[i]], axis=0).astype(jnp.bfloat16) for i in range(count)]


def pick_adapters(index, catalogs):
    per, rank, n = catalogs[0].shape[1:]

    def kernel(index_ref, *refs):
        sources, out_ref, sems = refs[:NX], refs[NX], refs[NX + 1]
        x = lax.axis_index("gx") % NX
        zl = lax.axis_index("gx") // NX
        for b in range(NY):
            a = index_ref[b]
            owner = a // per
            rx = (owner % NX - x + NX) % NX
            rz = (owner // NX - zl + ZL) % ZL
            for k in range(NX):

                @pl.when(rx == k)
                def _():
                    pltpu.make_async_copy(sources[k].at[rz, a % per], out_ref.at[b], sems.at[b]).start()

        for b in range(NY):
            pltpu.make_async_copy(sources[0].at[0, 0], out_ref.at[b], sems.at[b]).wait()

    return pl.pallas_call(
        kernel,
        in_specs=[smem()] + [hbm()] * NX,
        out_specs=hbm(),
        out_shape=jax.ShapeDtypeStruct((NY, rank, n), jnp.bfloat16),
        scratch_shapes=[pltpu.SemaphoreType.DMA((NY,))],
        compiler_params=params(),
        name="pick_adapters",
    )(index, *catalogs)


def finish(live, shrink_all, up, pieces):
    n = pieces[0].shape[1]

    def kernel(live_ref, shrink_ref, up_ref, *refs):
        ins, out_ref = refs[:ZL], refs[ZL]
        y = lax.axis_index("gy")
        zl = lax.axis_index("gx") // NX
        c = lax.axis_index("gz") % NC
        total = shrink_ref[0]
        for k in range(1, NY):
            total = total + shrink_ref[k]
        low = total.astype(jnp.bfloat16)
        mask = lax.broadcasted_iota(jnp.int32, (BLOCK, n), 0) < live_ref[y]
        cols = [zl, (zl + 1 + 2 * c) % ZL, (zl + 3 - 2 * c) % ZL, (zl + 2) % ZL]
        for col, piece in zip(cols, ins):
            expand = lax.dot_general(
                low, up_ref[col], (((0,), (0,)), ((), ())), preferred_element_type=jnp.float32
            )
            value = wide(piece[...]) + 2.0 * expand
            out_ref[:, pl.ds(pl.multiple_of(col * n, 128), n)] = jnp.where(mask, value, 0.0).astype(jnp.bfloat16)

    vmem = pl.BlockSpec(memory_space=pltpu.VMEM)
    return pl.pallas_call(
        kernel,
        in_specs=[smem()] + [vmem] * (2 + ZL),
        out_specs=vmem,
        out_shape=jax.ShapeDtypeStruct((BLOCK, n * ZL), jnp.bfloat16),
        compiler_params=params(),
        name="finish",
    )(live, shrink_all, up, *pieces)


def body(tokens, base_up_weight, adapter_down_weight, adapter_up_weight, block_adapter_index, request_rows):
    rows, width = tokens.shape
    y = lax.axis_index("gy")
    c = lax.axis_index("gz") % NC

    near = send(tokens, lambda z, x, c: ((z + 1 - 2 * c) % NZ, x, c))
    half = lax.dynamic_slice_in_dim(tokens, c * (rows // NC), rows // NC, 0)
    far = send(half, lambda z, x, c: ((z + 2 - 4 * c) % NZ, x, c))
    w_own = base_up_weight.T
    weights = [w_own] + [along_x(w_own, -r) for r in range(1, NX)]
    n = NX * w_own.shape[0]
    up_own = lax.dynamic_slice_in_dim(adapter_up_weight, y * n, n, 2)
    up_z = [up_own] + [
        send(up_own, lambda z, x, c, r=r: (within(z, -r), x, c)) for r in range(1, ZL)
    ]
    near_other = swap_cores(near)
    far_other = swap_cores(far)

    shrink_part = shrink(tokens, adapter_down_weight, block_adapter_index)
    shrink_all = lax.all_to_all(shrink_part, "gy", 0, 0, tiled=True)

    weights, near, near_other, far, far_other, up_z, shrink_all = lax.optimization_barrier(
        (weights, near, near_other, far, far_other, up_z, shrink_all)
    )
    first = partial_products([(near,), (far, far_other)], weights)
    got_first = step_one(first)
    second = partial_products([(near_other,), (tokens,)], weights)
    got_second = step_one(second)
    got_first, _ = lax.optimization_barrier((got_first, second[4]))
    sum_near, sum_far = summed(first, got_first, step_two(first, got_first))
    sum_other, sum_own = summed(second, got_second, step_two(second, got_second))
    piece_near = send(sum_near, lambda z, x, c: (within(z, 2 * c - 1), x, c))
    piece_far = send(sum_far, lambda z, x, c: (within(z, 2), x, c))
    piece_other = send(sum_other, lambda z, x, c: (within(z, 1 - 2 * c), x, c))

    up_z = jnp.stack(up_z)
    catalogs = [up_z] + [along_x(up_z, -r) for r in range(1, NX)]
    picked = pick_adapters(block_adapter_index, catalogs)
    up = lax.all_to_all(picked, "gy", 0, 0, tiled=True)
    return finish(request_rows, shrink_all, up, (sum_own, piece_near, piece_other, piece_far))


def solution(mesh):
    in_specs = (
        P("gx", "gy"),
        P("gy", ("gz", "gx")),
        P(None, None, "gy"),
        P("gx", None, "gz"),
        P("gx"),
        P("gx"),
    )
    out_specs = P(("gx", "gy"), "gz")
    return jax.shard_map(body, mesh=mesh, in_specs=in_specs, out_specs=out_specs, check_vma=False)
```

```python
import jax
import jax.numpy as jnp
from jax import lax
from jax.experimental import pallas as pl
from jax.experimental.pallas import tpu as pltpu
from jax.sharding import PartitionSpec as P


BLOCK = 128
ZL, NX, NY, ZH, NC = 4, 4, 4, 2, 2
TERMS = 3
NZ = ZL * ZH
VMEM_LIMIT = 48 * 2**20


def device_perm(move):
    def place(z, x, c):
        return (z % ZL * NX + x) * ZH * NC + z // ZL * NC + c

    return [(place(z, x, c), place(*move(z, x, c))) for z in range(NZ) for x in range(NX) for c in range(NC)]


def send(a, move):
    return lax.ppermute(a, ("gx", "gz"), device_perm(move))


def within(z, shift):
    return z // ZL * ZL + (z + shift) % ZL


def along_x(a, shift):
    return lax.ppermute(a, "gx", [(z * NX + x, z * NX + (x + shift) % NX) for z in range(ZL) for x in range(NX)])


def along_y(a, shift):
    return lax.ppermute(a, "gy", [(y, (y + shift) % NY) for y in range(NY)])


def swap_cores(a):
    return send(a, lambda z, x, c: (z, x, 1 - c))


def nt_dot(a, b):
    return lax.dot_general(a, b, (((1,), (1,)), ((), ())), preferred_element_type=jnp.float32)


def hbm():
    return pl.BlockSpec(memory_space=pltpu.HBM)


def smem():
    return pl.BlockSpec(memory_space=pltpu.SMEM)


def params():
    return pltpu.CompilerParams(vmem_limit_bytes=VMEM_LIMIT)


def shrink(tokens, down, index):
    rank, width = down.shape[1:]

    def kernel(index_ref, tok_hbm, down_hbm, *refs):
        outs, (tok_ref, down_ref, out_ref, sems) = refs[:NY], refs[NY:]
        y = lax.axis_index("gy")
        loads = [pltpu.make_async_copy(tok_hbm, tok_ref, sems.at[0])]
        for b in range(NY):
            loads.append(pltpu.make_async_copy(down_hbm.at[index_ref[b]], down_ref.at[b], sems.at[1 + b]))
        for copy in loads:
            copy.start()
        for copy in loads:
            copy.wait()
        for b in range(NY):
            rest = nt_dot(down_ref[b], tok_ref[pl.ds(b * BLOCK, BLOCK), :])
            for term in range(TERMS):
                part = rest.astype(jnp.bfloat16)
                out_ref[b, :, term * BLOCK : (term + 1) * BLOCK] = part
                rest = rest - part.astype(jnp.float32)
        stores = [
            pltpu.make_async_copy(out_ref.at[(y + k) % NY], outs[k], sems.at[k]) for k in range(NY)
        ]
        for copy in stores:
            copy.start()
        for copy in stores:
            copy.wait()

    return pl.pallas_call(
        kernel,
        in_specs=[smem(), hbm(), hbm()],
        out_specs=[hbm()] * NY,
        out_shape=[jax.ShapeDtypeStruct((rank, TERMS * BLOCK), jnp.bfloat16)] * NY,
        scratch_shapes=[
            pltpu.VMEM(tokens.shape, jnp.bfloat16),
            pltpu.VMEM((NY, rank, width), jnp.bfloat16),
            pltpu.VMEM((NY, rank, TERMS * BLOCK), jnp.bfloat16),
            pltpu.SemaphoreType.DMA((1 + NY,)),
        ],
        compiler_params=params(),
        name="shrink",
    )(index, tokens, down)


def partial_products(chunks, weight_sets):
    weights = [w for pieces in weight_sets for w in pieces]
    width = weights[0].shape[1]
    n = sum(w.shape[0] for w in weights)
    count = len(chunks)
    rows = NY * BLOCK
    flat = [a for chunk in chunks for a in chunk]
    sizes = [len(chunk) for chunk in chunks]
    half = BLOCK // 2

    def kernel(*refs):
        ins, w_in = refs[: len(flat)], refs[len(flat) : len(flat) + len(weights)]
        outs = refs[len(flat) + len(weights) : len(flat) + len(weights) + 5]
        t_ref, w_ref, o_ref, in_sems, w_sem, out_sems = refs[len(flat) + len(weights) + 5 :]
        x = lax.axis_index("gx") % NX
        y = lax.axis_index("gy")
        c = lax.axis_index("gz") % NC
        w_copies, base = [], 0
        for i, w in enumerate(weights):
            nb = w.shape[0]
            at = pl.multiple_of(base + (x + i % NX) % NX * nb, 32)
            w_copies.append(pltpu.make_async_copy(w_in[i], w_ref.at[pl.ds(at, nb), :], w_sem))
            if i % NX == NX - 1:
                base += NX * nb
        t_copies, at = [], 0
        for i, size in enumerate(sizes):
            part = rows // size
            for j in range(size):
                start = i * rows + (j if size == 1 else (c + j) % NC) * part
                t_copies.append(
                    pltpu.make_async_copy(
                        ins[at], t_ref.at[pl.ds(pl.multiple_of(start, BLOCK), part), :], in_sems.at[i]
                    )
                )
                at += 1
        for copy in t_copies[: sizes[0]] + w_copies + t_copies[sizes[0] :]:
            copy.start()
        pltpu.make_async_copy(w_ref, w_ref, w_sem).wait()

        def moves(i):
            def rows_of(shift, low, size):
                start = i * rows + (y + shift) % NY * BLOCK + low
                return o_ref.at[pl.ds(pl.multiple_of(start, half), size), :]

            def at(k, start, size):
                return outs[k].at[pl.ds(pl.multiple_of(start, half), size), :]

            pairs = [
                (rows_of(2, 0, half), at(1, i * BLOCK, half)),
                (rows_of(1, half, half), at(1, i * BLOCK + half, half)),
                (rows_of(3, 0, half), at(2, i * BLOCK, half)),
                (rows_of(2, half, half), at(2, i * BLOCK + half, half)),
                (rows_of(1, 0, half), at(3, i * half, half)),
                (rows_of(3, half, half), at(4, i * half, half)),
                (rows_of(0, 0, BLOCK), at(0, i * BLOCK, BLOCK)),
            ]
            return [pltpu.make_async_copy(src, dst, out_sems.at[i, k]) for k, (src, dst) in enumerate(pairs)]

        def step(i, carry):
            mine = pl.ds(pl.multiple_of(i * rows, rows), rows)
            pltpu.make_async_copy(t_ref.at[mine, :], t_ref.at[mine, :], in_sems.at[i]).wait()
            o_ref[mine, :] = nt_dot(t_ref[mine, :], w_ref[...]).astype(jnp.bfloat16)
            for copy in moves(i):
                copy.start()
            return carry

        lax.fori_loop(0, count, step, 0)

        def drain(i, carry):
            for copy in moves(i):
                copy.wait()
            return carry

        lax.fori_loop(0, count, drain, 0)

    def out(m):
        return jax.ShapeDtypeStruct((m * count, n), jnp.bfloat16)

    return pl.pallas_call(
        kernel,
        in_specs=[hbm()] * (len(flat) + len(weights)),
        out_specs=[hbm()] * 5,
        out_shape=[out(BLOCK)] * 3 + [out(half)] * 2,
        scratch_shapes=[
            pltpu.VMEM((count * rows, width), jnp.bfloat16),
            pltpu.VMEM((n, width), jnp.bfloat16),
            pltpu.VMEM((count * rows, n), jnp.bfloat16),
            pltpu.SemaphoreType.DMA((count,)),
            pltpu.SemaphoreType.DMA,
            pltpu.SemaphoreType.DMA((count, 7)),
        ],
        cost_estimate=pl.CostEstimate(
            flops=2 * count * rows * width * n,
            bytes_accessed=2 * (count * rows * width + width * n + count * rows * n),
            transcendentals=0,
        ),
        compiler_params=params(),
        name="partial_products",
    )(*flat, *weights)


def wide(a):
    return a.astype(jnp.float32)


def step_one(parts):
    _, plus, minus, _, _ = parts
    from_minus = along_y(plus, 1)
    return from_minus, along_y(minus, -1)


def step_two(parts, first):
    half = BLOCK // 2
    own, _, _, plus, minus = parts
    count, n = own.shape[0] // BLOCK, own.shape[1]
    from_minus, from_plus = (a.reshape(count, 2, half, n) for a in first)
    plus, minus = plus.reshape(count, half, n), minus.reshape(count, half, n)
    to_plus = (wide(plus) + wide(from_minus[:, 0])).astype(jnp.bfloat16)
    to_minus = (wide(minus) + wide(from_plus[:, 1])).astype(jnp.bfloat16)
    a = along_y(to_plus, 1)
    return a, along_y(to_minus, -1)


def summed(parts, first, second):
    half = BLOCK // 2
    own = parts[0]
    count, n = own.shape[0] // BLOCK, own.shape[1]
    from_minus, from_plus = (a.reshape(count, 2, half, n) for a in first)
    own = own.reshape(count, 2, half, n)
    low = wide(own[:, 0]) + wide(from_plus[:, 0]) + wide(second[0])
    high = wide(own[:, 1]) + wide(from_minus[:, 1]) + wide(second[1])
    return [jnp.concatenate([low[i], high[i]], axis=0).astype(jnp.bfloat16) for i in range(count)]


def pick_adapters(index, catalogs, shrinks):
    per, rank, n = catalogs[0].shape[1:]

    def kernel(index_ref, *refs):
        sources, terms, outs, sems = refs[:NX], refs[NX : NX + NY], refs[NX + NY : NX + 2 * NY], refs[NX + 2 * NY]
        for b in range(NY):
            pltpu.make_async_copy(terms[b], outs[b].at[:, n:], sems.at[NY + b]).start()
        x = lax.axis_index("gx") % NX
        zl = lax.axis_index("gx") // NX
        y = lax.axis_index("gy")
        for b in range(NY):
            a = index_ref[(y + b) % NY]
            owner = a // per
            rx = (owner % NX - x + NX) % NX
            rz = (owner // NX - zl + ZL) % ZL
            for k in range(NX):

                @pl.when(rx == k)
                def _():
                    pltpu.make_async_copy(sources[k].at[rz, a % per], outs[b].at[:, :n], sems.at[b]).start()

        for b in range(NY):
            pltpu.make_async_copy(sources[0].at[0, 0], outs[b].at[:, :n], sems.at[b]).wait()
            pltpu.make_async_copy(terms[b], outs[b].at[:, n:], sems.at[NY + b]).wait()

    return pl.pallas_call(
        kernel,
        in_specs=[smem()] + [hbm()] * (NX + NY),
        out_specs=[hbm()] * NY,
        out_shape=[jax.ShapeDtypeStruct((rank, n + shrinks[0].shape[1]), jnp.bfloat16)] * NY,
        scratch_shapes=[pltpu.SemaphoreType.DMA((2 * NY,))],
        compiler_params=params(),
        name="pick_adapters",
    )(index, *catalogs, *shrinks)


def finish(live, ups, pieces):
    rank = ups[0].shape[0]
    n = ups[0].shape[1] - TERMS * BLOCK
    flat = [a for parts in pieces for a in parts]

    def kernel(live_ref, *refs):
        up_refs, ins, out_ref, up_ref = refs[:NY], list(refs[NY:-2]), refs[-2], refs[-1]
        y = lax.axis_index("gy")
        zl = lax.axis_index("gx") // NX
        c = lax.axis_index("gz") % NC
        total = jnp.zeros((rank, BLOCK), jnp.float32)
        for k in range(NY):
            for term in range(TERMS):
                total = total + wide(up_refs[k][:, n + term * BLOCK : n + (term + 1) * BLOCK])
            up_ref[(y - k + NY) % NY] = up_refs[k][:, :n]
        low = total.astype(jnp.bfloat16)
        mask = lax.broadcasted_iota(jnp.int32, (BLOCK, n), 0) < live_ref[y]
        cols = [zl, (zl + 1 + 2 * c) % ZL, (zl + 3 - 2 * c) % ZL, (zl + 2) % ZL]
        for col, parts in zip(cols, pieces):
            refs_here = [ins.pop(0) for _ in parts]
            halves = [(refs_here[0], 0, FIRST)]
            halves.append((refs_here[-1], 0 if len(parts) == 2 else NX * FIRST, n // NX - FIRST))
            expand = lax.dot_general(
                low, up_ref[col], (((0,), (0,)), ((), ())), preferred_element_type=jnp.float32
            )
            blocks = [
                ref[:, base + x * size : base + (x + 1) * size] for x in range(NX) for ref, base, size in halves
            ]
            value = wide(jnp.concatenate(blocks, axis=1)) + 2.0 * expand
            out_ref[:, pl.ds(pl.multiple_of(col * n, 128), n)] = jnp.where(mask, value, 0.0).astype(jnp.bfloat16)

    vmem = pl.BlockSpec(memory_space=pltpu.VMEM)
    return pl.pallas_call(
        kernel,
        in_specs=[smem()] + [vmem] * (NY + len(flat)),
        out_specs=vmem,
        out_shape=jax.ShapeDtypeStruct((BLOCK, n * ZL), jnp.bfloat16),
        scratch_shapes=[pltpu.VMEM((NY, rank, n), jnp.bfloat16)],
        compiler_params=params(),
        name="finish",
    )(live, *ups, *flat)


FIRST = 128


def layer(tokens, base_up_weight, adapter_down_weight, adapter_up_weight, block_adapter_index, request_rows):
    rows, _ = tokens.shape
    y = lax.axis_index("gy")
    c = lax.axis_index("gz") % NC

    near = send(tokens, lambda z, x, c: ((z + 1 - 2 * c) % NZ, x, c))
    weights = []
    for part in (base_up_weight[:, :FIRST], base_up_weight[:, FIRST:]):
        pieces = [part.T]
        for r in range(1, NX):
            pieces.append(along_x(pieces[0], -r))
        weights.append(pieces)
    half = lax.dynamic_slice_in_dim(tokens, c * (rows // NC), rows // NC, 0)
    far = send(half, lambda z, x, c: ((z + 2 - 4 * c) % NZ, x, c))
    n = NX * base_up_weight.shape[1]
    up_z = [lax.dynamic_slice_in_dim(adapter_up_weight, y * n, n, 2)]
    for r in range(1, ZL):
        up_z.append(send(up_z[0], lambda z, x, c, r=r: (within(z, -r), x, c)))
    other = swap_cores(near)
    far_other = swap_cores(far)

    a = partial_products([(tokens,), (near,)], weights[:1])
    a1 = step_one(a)
    b = partial_products([(other,), (far, far_other)], weights)
    b1 = step_one(b)
    a2 = step_two(a, a1)
    d = partial_products([(tokens,), (near,)], weights[1:])
    d1 = step_one(d)
    own0, near0 = summed(a, a1, a2)
    b2 = step_two(b, b1)
    d2 = step_two(d, d1)
    other, far = summed(b, b1, b2)
    own1, near1 = summed(d, d1, d2)

    def to_near(z, x, c):
        return within(z, 2 * c - 1), x, c

    near0 = send(near0, to_near)
    far = send(far, lambda z, x, c: (within(z, 2), x, c))
    other = send(other, lambda z, x, c: (within(z, 1 - 2 * c), x, c))
    near1 = send(near1, to_near)

    shrinks = shrink(tokens, adapter_down_weight, block_adapter_index)
    up_z = jnp.stack(up_z)
    catalogs = [up_z]
    for r in range(1, NX):
        catalogs.append(along_x(up_z, -r))
    ups = list(pick_adapters(block_adapter_index, catalogs, shrinks))
    for k in range(1, NY):
        ups[k] = along_y(ups[k], k)
    return finish(request_rows, ups, ((own0, own1), (near0, near1), (other,), (far,)))


def solution(mesh):
    in_specs = (
        P("gx", "gy"),
        P("gy", ("gz", "gx")),
        P(None, None, "gy"),
        P("gx", None, "gz"),
        P("gx"),
        P("gx"),
    )
    out_specs = P(("gx", "gy"), "gz")
    return jax.shard_map(layer, mesh=mesh, in_specs=in_specs, out_specs=out_specs, check_vma=False)
```

```python
import jax
import jax.numpy as jnp
from jax import lax
from jax.experimental import pallas as pl
from jax.experimental.pallas import tpu as pltpu
from jax.sharding import PartitionSpec as P


BLOCK = 128
ZL, NX, NY, ZH, NC = 4, 4, 4, 2, 2
TERMS = 3
NZ = ZL * ZH
VMEM_LIMIT = 48 * 2**20


def device_perm(move):
    def place(z, x, c):
        return (z % ZL * NX + x) * ZH * NC + z // ZL * NC + c

    return [(place(z, x, c), place(*move(z, x, c))) for z in range(NZ) for x in range(NX) for c in range(NC)]


def send(a, move):
    return lax.ppermute(a, ("gx", "gz"), device_perm(move))


def within(z, shift):
    return z // ZL * ZL + (z + shift) % ZL


def along_x(a, shift):
    return lax.ppermute(a, "gx", [(z * NX + x, z * NX + (x + shift) % NX) for z in range(ZL) for x in range(NX)])


def along_y(a, shift):
    return lax.ppermute(a, "gy", [(y, (y + shift) % NY) for y in range(NY)])


def swap_cores(a):
    return send(a, lambda z, x, c: (z, x, 1 - c))


def nt_dot(a, b):
    return lax.dot_general(a, b, (((1,), (1,)), ((), ())), preferred_element_type=jnp.float32)


def hbm():
    return pl.BlockSpec(memory_space=pltpu.HBM)


def smem():
    return pl.BlockSpec(memory_space=pltpu.SMEM)


def params():
    return pltpu.CompilerParams(vmem_limit_bytes=VMEM_LIMIT)


def shrink(tokens, down, index):
    rank, width = down.shape[1:]

    def kernel(index_ref, tok_hbm, down_hbm, *refs):
        outs, (tok_ref, down_ref, out_ref, sems) = refs[:NY], refs[NY:]
        y = lax.axis_index("gy")
        loads = [pltpu.make_async_copy(tok_hbm, tok_ref, sems.at[0])]
        for b in range(NY):
            loads.append(pltpu.make_async_copy(down_hbm.at[index_ref[b]], down_ref.at[b], sems.at[1 + b]))
        for copy in loads:
            copy.start()
        for copy in loads:
            copy.wait()
        for b in range(NY):
            rest = nt_dot(down_ref[b], tok_ref[pl.ds(b * BLOCK, BLOCK), :])
            for term in range(TERMS):
                part = rest.astype(jnp.bfloat16)
                out_ref[b, :, term * BLOCK : (term + 1) * BLOCK] = part
                rest = rest - part.astype(jnp.float32)
        stores = [
            pltpu.make_async_copy(out_ref.at[(y + k) % NY], outs[k], sems.at[k]) for k in range(NY)
        ]
        for copy in stores:
            copy.start()
        for copy in stores:
            copy.wait()

    return pl.pallas_call(
        kernel,
        in_specs=[smem(), hbm(), hbm()],
        out_specs=[hbm()] * NY,
        out_shape=[jax.ShapeDtypeStruct((rank, TERMS * BLOCK), jnp.bfloat16)] * NY,
        scratch_shapes=[
            pltpu.VMEM(tokens.shape, jnp.bfloat16),
            pltpu.VMEM((NY, rank, width), jnp.bfloat16),
            pltpu.VMEM((NY, rank, TERMS * BLOCK), jnp.bfloat16),
            pltpu.SemaphoreType.DMA((1 + NY,)),
        ],
        compiler_params=params(),
        name="shrink",
    )(index, tokens, down)


def partial_products(items, weight_sets):
    weights = [w for pieces in weight_sets for w in pieces]
    width = weights[0].shape[1]
    set_rows = [NX * pieces[0].shape[0] for pieces in weight_sets]
    total = sum(set_rows)
    rows = NY * BLOCK
    flat = [a for arrays, _, _ in items for a in arrays]
    spans, n = [], 0
    for _, lo, hi in items:
        spans.append((sum(set_rows[:lo]), sum(set_rows[lo:hi]), n))
        n += spans[-1][1]
    half = BLOCK // 2
    part = rows // 2

    def kernel(*refs):
        ins, w_in = refs[: len(flat)], refs[len(flat) : len(flat) + len(weights)]
        outs = refs[len(flat) + len(weights) : len(flat) + len(weights) + 5]
        t_ref, w_ref, o_ref, in_sems, w_sem, out_sems = refs[len(flat) + len(weights) + 5 :]
        x = lax.axis_index("gx") % NX
        y = lax.axis_index("gy")
        c = lax.axis_index("gz") % NC
        w_copies, base = [], 0
        for i, w in enumerate(weights):
            nb = w.shape[0]
            at = pl.multiple_of(base + (x + i % NX) % NX * nb, 32)
            w_copies.append(pltpu.make_async_copy(w_in[i], w_ref.at[pl.ds(at, nb), :], w_sem))
            if i % NX == NX - 1:
                base += NX * nb
        t_copies, at = [], 0
        for i, (arrays, _, _) in enumerate(items):
            for j, array in enumerate(arrays):
                size = array.shape[0]
                start = (j if len(arrays) == 1 else (c + j) % NC) * size
                dst = t_ref.at[i, pl.ds(pl.multiple_of(start, BLOCK), size), :]
                t_copies.append(pltpu.make_async_copy(ins[at], dst, in_sems.at[i]))
                at += 1
        first = len(items[0][0])
        for copy in t_copies[:first] + w_copies + t_copies[first:]:
            copy.start()
        pltpu.make_async_copy(w_ref, w_ref, w_sem).wait()
        done = []
        for i, (low, size, col) in enumerate(spans):
            pltpu.make_async_copy(t_ref.at[i], t_ref.at[i], in_sems.at[i]).wait()
            lanes = pl.ds(col, size)

            def step(j, carry):
                mine = pl.ds(pl.multiple_of(j * part, part), part)
                o_ref[mine, lanes] = nt_dot(t_ref[i, mine, :], w_ref[pl.ds(low, size), :]).astype(jnp.bfloat16)
                return carry

            lax.fori_loop(0, rows // part, step, 0)

            def rows_of(shift, low, size):
                start = (y + shift) % NY * BLOCK + low
                return o_ref.at[pl.ds(pl.multiple_of(start, half), size), lanes]

            pairs = [
                (rows_of(2, 0, half), outs[1].at[:half, lanes]),
                (rows_of(1, half, half), outs[1].at[half:, lanes]),
                (rows_of(3, 0, half), outs[2].at[:half, lanes]),
                (rows_of(2, half, half), outs[2].at[half:, lanes]),
                (rows_of(1, 0, half), outs[3].at[:, lanes]),
                (rows_of(3, half, half), outs[4].at[:, lanes]),
                (rows_of(0, 0, BLOCK), outs[0].at[:, lanes]),
            ]
            for k, (src, dst) in enumerate(pairs):
                done.append(pltpu.make_async_copy(src, dst, out_sems.at[i, k]))
                done[-1].start()
        for copy in done:
            copy.wait()

    def out(m):
        return jax.ShapeDtypeStruct((m, n), jnp.bfloat16)

    return pl.pallas_call(
        kernel,
        in_specs=[hbm()] * (len(flat) + len(weights)),
        out_specs=[hbm()] * 5,
        out_shape=[out(BLOCK)] * 3 + [out(half)] * 2,
        scratch_shapes=[
            pltpu.VMEM((len(items), rows, width), jnp.bfloat16),
            pltpu.VMEM((total, width), jnp.bfloat16),
            pltpu.VMEM((rows, n), jnp.bfloat16),
            pltpu.SemaphoreType.DMA((len(items),)),
            pltpu.SemaphoreType.DMA,
            pltpu.SemaphoreType.DMA((len(items), 7)),
        ],
        cost_estimate=pl.CostEstimate(
            flops=2 * rows * width * n,
            bytes_accessed=2 * (len(items) * rows * width + width * total + rows * n),
            transcendentals=0,
        ),
        compiler_params=params(),
        name="partial_products",
    )(*flat, *weights)


def wide(a):
    return a.astype(jnp.float32)


def step_one(parts):
    _, plus, minus, _, _ = parts
    from_minus = along_y(plus, 1)
    return from_minus, along_y(minus, -1)


def step_two(parts, first):
    half = BLOCK // 2
    _, _, _, plus, minus = parts
    from_minus, from_plus = first
    to_plus = (wide(plus) + wide(from_minus[:half])).astype(jnp.bfloat16)
    to_minus = (wide(minus) + wide(from_plus[half:])).astype(jnp.bfloat16)
    a = along_y(to_plus, 1)
    return a, along_y(to_minus, -1)


def summed(parts, first, second):
    half = BLOCK // 2
    own = parts[0]
    from_minus, from_plus = first
    low = wide(own[:half]) + wide(from_plus[:half]) + wide(second[0])
    high = wide(own[half:]) + wide(from_minus[half:]) + wide(second[1])
    return jnp.concatenate([low, high], axis=0).astype(jnp.bfloat16)


def pick_adapters(index, catalogs, shrinks):
    per, rank, n = catalogs[0].shape[1:]

    def kernel(index_ref, *refs):
        sources, terms, outs, sems = refs[:NX], refs[NX : NX + NY], refs[NX + NY : NX + 2 * NY], refs[NX + 2 * NY]
        for b in range(NY):
            pltpu.make_async_copy(terms[b], outs[b].at[:, n:], sems.at[NY + b]).start()
        x = lax.axis_index("gx") % NX
        zl = lax.axis_index("gx") // NX
        y = lax.axis_index("gy")
        for b in range(NY):
            a = index_ref[(y + b) % NY]
            owner = a // per
            rx = (owner % NX - x + NX) % NX
            rz = (owner // NX - zl + ZL) % ZL
            for k in range(NX):

                @pl.when(rx == k)
                def _():
                    pltpu.make_async_copy(sources[k].at[rz, a % per], outs[b].at[:, :n], sems.at[b]).start()

        for b in range(NY):
            pltpu.make_async_copy(sources[0].at[0, 0], outs[b].at[:, :n], sems.at[b]).wait()
            pltpu.make_async_copy(terms[b], outs[b].at[:, n:], sems.at[NY + b]).wait()

    return pl.pallas_call(
        kernel,
        in_specs=[smem()] + [hbm()] * (NX + NY),
        out_specs=[hbm()] * NY,
        out_shape=[jax.ShapeDtypeStruct((rank, n + shrinks[0].shape[1]), jnp.bfloat16)] * NY,
        scratch_shapes=[pltpu.SemaphoreType.DMA((2 * NY,))],
        compiler_params=params(),
        name="pick_adapters",
    )(index, *catalogs, *shrinks)


def finish(live, ups, pieces):
    rank = ups[0].shape[0]
    n = ups[0].shape[1] - TERMS * BLOCK
    flat = [a for parts in pieces for a in parts]

    def kernel(live_ref, *refs):
        up_refs, ins, out_ref, up_ref = refs[:NY], list(refs[NY:-2]), refs[-2], refs[-1]
        y = lax.axis_index("gy")
        zl = lax.axis_index("gx") // NX
        c = lax.axis_index("gz") % NC
        total = jnp.zeros((rank, BLOCK), jnp.float32)
        for k in range(NY):
            for term in range(TERMS):
                total = total + wide(up_refs[k][:, n + term * BLOCK : n + (term + 1) * BLOCK])
            up_ref[(y - k + NY) % NY] = up_refs[k][:, :n]
        low = total.astype(jnp.bfloat16)
        mask = lax.broadcasted_iota(jnp.int32, (BLOCK, n), 0) < live_ref[y]
        cols = [zl, (zl + 1 + 2 * c) % ZL, (zl + 3 - 2 * c) % ZL, (zl + 2) % ZL]
        for col, parts in zip(cols, pieces):
            refs_here = [ins.pop(0) for _ in parts]
            halves = [(refs_here[0], 0, FIRST)]
            halves.append((refs_here[-1], 0 if len(parts) == 2 else NX * FIRST, n // NX - FIRST))
            expand = lax.dot_general(
                low, up_ref[col], (((0,), (0,)), ((), ())), preferred_element_type=jnp.float32
            )
            blocks = [
                ref[:, base + x * size : base + (x + 1) * size] for x in range(NX) for ref, base, size in halves
            ]
            value = wide(jnp.concatenate(blocks, axis=1)) + 2.0 * expand
            out_ref[:, pl.ds(pl.multiple_of(col * n, 128), n)] = jnp.where(mask, value, 0.0).astype(jnp.bfloat16)

    vmem = pl.BlockSpec(memory_space=pltpu.VMEM)
    return pl.pallas_call(
        kernel,
        in_specs=[smem()] + [vmem] * (NY + len(flat)),
        out_specs=vmem,
        out_shape=jax.ShapeDtypeStruct((BLOCK, n * ZL), jnp.bfloat16),
        scratch_shapes=[pltpu.VMEM((NY, rank, n), jnp.bfloat16)],
        compiler_params=params(),
        name="finish",
    )(live, *ups, *flat)


FIRST = 160


def layer(tokens, base_up_weight, adapter_down_weight, adapter_up_weight, block_adapter_index, request_rows):
    rows, _ = tokens.shape
    y = lax.axis_index("gy")
    c = lax.axis_index("gz") % NC

    near = send(tokens, lambda z, x, c: ((z + 1 - 2 * c) % NZ, x, c))
    weights = []
    for part in (base_up_weight[:, :FIRST], base_up_weight[:, FIRST:]):
        pieces = [part.T]
        for r in range(1, NX):
            pieces.append(along_x(pieces[0], -r))
        weights.append(pieces)
    half = lax.dynamic_slice_in_dim(tokens, c * (rows // NC), rows // NC, 0)
    far = send(half, lambda z, x, c: ((z + 2 - 4 * c) % NZ, x, c))
    n = NX * base_up_weight.shape[1]
    up_z = [lax.dynamic_slice_in_dim(adapter_up_weight, y * n, n, 2)]
    for r in range(1, ZL):
        up_z.append(send(up_z[0], lambda z, x, c, r=r: (within(z, -r), x, c)))
    other = swap_cores(near)
    far_other = swap_cores(far)

    a = partial_products([((near,), 0, 1), ((other,), 0, 1)], weights[:1])
    a1 = step_one(a)
    b = partial_products([((near,), 1, 2), ((far, far_other), 0, 2)], weights)
    b1 = step_one(b)
    a2 = step_two(a, a1)
    d = partial_products([((other,), 1, 2), ((tokens,), 0, 2)], weights)
    b2 = step_two(b, b1)
    d1 = step_one(d)
    cut, rest = NX * FIRST, n - NX * FIRST
    sum_a = summed(a, a1, a2)
    sum_b = summed(b, b1, b2)
    d2 = step_two(d, d1)
    sum_d = summed(d, d1, d2)

    def to_near(z, x, c):
        return within(z, 2 * c - 1), x, c

    def to_other(z, x, c):
        return within(z, 1 - 2 * c), x, c

    near0 = send(sum_a[:, :cut], to_near)
    other0 = send(sum_a[:, cut:], to_other)
    far = send(sum_b[:, rest:], lambda z, x, c: (within(z, 2), x, c))
    near1 = send(sum_b[:, :rest], to_near)
    other1 = send(sum_d[:, :rest], to_other)
    own = sum_d[:, rest:]

    shrinks = shrink(tokens, adapter_down_weight, block_adapter_index)
    up_z = jnp.stack(up_z)
    catalogs = [up_z]
    for r in range(1, NX):
        catalogs.append(along_x(up_z, -r))
    ups = list(pick_adapters(block_adapter_index, catalogs, shrinks))
    for k in range(1, NY):
        ups[k] = along_y(ups[k], k)
    return finish(request_rows, ups, ((own,), (near0, near1), (other0, other1), (far,)))


def solution(mesh):
    in_specs = (
        P("gx", "gy"),
        P("gy", ("gz", "gx")),
        P(None, None, "gy"),
        P("gx", None, "gz"),
        P("gx"),
        P("gx"),
    )
    out_specs = P(("gx", "gy"), "gz")
    return jax.shard_map(layer, mesh=mesh, in_specs=in_specs, out_specs=out_specs, check_vma=False)
```

```python
import jax
import jax.numpy as jnp
from jax import lax
from jax.experimental import pallas as pl
from jax.experimental.pallas import tpu as pltpu
from jax.sharding import PartitionSpec as P


BLOCK = 128
ZL, NX, NY, ZH, NC = 4, 4, 4, 2, 2
TERMS = 3
NZ = ZL * ZH
VMEM_LIMIT = 16 * 2**20


def device_perm(move):
    def place(z, x, c):
        return (z % ZL * NX + x) * ZH * NC + z // ZL * NC + c

    return [(place(z, x, c), place(*move(z, x, c))) for z in range(NZ) for x in range(NX) for c in range(NC)]


def send(a, move):
    return lax.ppermute(a, ("gx", "gz"), device_perm(move))


def within(z, shift):
    return z // ZL * ZL + (z + shift) % ZL


def along_x(a, shift):
    return lax.ppermute(a, "gx", [(z * NX + x, z * NX + (x + shift) % NX) for z in range(ZL) for x in range(NX)])


def along_y(a, shift):
    return lax.ppermute(a, "gy", [(y, (y + shift) % NY) for y in range(NY)])


def swap_cores(a):
    return send(a, lambda z, x, c: (z, x, 1 - c))


def nt_dot(a, b):
    return lax.dot_general(a, b, (((1,), (1,)), ((), ())), preferred_element_type=jnp.float32)


def hbm():
    return pl.BlockSpec(memory_space=pltpu.HBM)


def smem():
    return pl.BlockSpec(memory_space=pltpu.SMEM)


def params():
    return pltpu.CompilerParams(vmem_limit_bytes=VMEM_LIMIT)


def shrink(tokens, down, index):
    rank, width = down.shape[1:]

    def kernel(index_ref, tok_hbm, down_hbm, *refs):
        outs, (tok_ref, down_ref, out_ref, sems) = refs[:NY], refs[NY:]
        y = lax.axis_index("gy")
        loads = [pltpu.make_async_copy(tok_hbm, tok_ref, sems.at[0])]
        for b in range(NY):
            loads.append(pltpu.make_async_copy(down_hbm.at[index_ref[b]], down_ref.at[b], sems.at[1 + b]))
        for copy in loads:
            copy.start()
        for copy in loads:
            copy.wait()
        for b in range(NY):
            rest = nt_dot(down_ref[b], tok_ref[pl.ds(b * BLOCK, BLOCK), :])
            for term in range(TERMS):
                part = rest.astype(jnp.bfloat16)
                out_ref[b, :, term * BLOCK : (term + 1) * BLOCK] = part
                rest = rest - part.astype(jnp.float32)
        stores = [
            pltpu.make_async_copy(out_ref.at[(y + k) % NY], outs[k], sems.at[k]) for k in range(NY)
        ]
        for copy in stores:
            copy.start()
        for copy in stores:
            copy.wait()

    return pl.pallas_call(
        kernel,
        in_specs=[smem(), hbm(), hbm()],
        out_specs=[hbm()] * NY,
        out_shape=[jax.ShapeDtypeStruct((rank, TERMS * BLOCK), jnp.bfloat16)] * NY,
        scratch_shapes=[
            pltpu.VMEM(tokens.shape, jnp.bfloat16),
            pltpu.VMEM((NY, rank, width), jnp.bfloat16),
            pltpu.VMEM((NY, rank, TERMS * BLOCK), jnp.bfloat16),
            pltpu.SemaphoreType.DMA((1 + NY,)),
        ],
        compiler_params=params(),
        name="shrink",
    )(index, tokens, down)


def partial_products(items, weight_sets, direct=False):
    weights = [w for pieces in weight_sets for w in pieces]
    width = weights[0].shape[1]
    set_rows = [NX * pieces[0].shape[0] for pieces in weight_sets]
    total = sum(set_rows)
    rows = NY * BLOCK
    flat = [a for arrays, _, _ in items for a in arrays]
    spans, n = [], 0
    for _, lo, hi in items:
        spans.append((sum(set_rows[:lo]), sum(set_rows[lo:hi]), n))
        n += spans[-1][1]
    half = BLOCK // 2
    part = rows // 2

    def kernel(*refs):
        ins, w_in = refs[: len(flat)], refs[len(flat) : len(flat) + len(weights)]
        outs = refs[len(flat) + len(weights) : -6]
        t_ref, w_ref, o_ref, in_sems, w_sem, out_sems = refs[-6:]
        x = lax.axis_index("gx") % NX
        y = lax.axis_index("gy")
        c = lax.axis_index("gz") % NC
        w_copies, base = [], 0
        for i, w in enumerate(weights):
            nb = w.shape[0]
            at = pl.multiple_of(base + (x + i % NX) % NX * nb, 32)
            w_copies.append(pltpu.make_async_copy(w_in[i], w_ref.at[pl.ds(at, nb), :], w_sem))
            if i % NX == NX - 1:
                base += NX * nb
        t_copies, at = [], 0
        for i, (arrays, _, _) in enumerate(items):
            for j, array in enumerate(arrays):
                size = array.shape[0]
                start = (j if len(arrays) == 1 else (c + j) % NC) * size
                dst = t_ref.at[i, pl.ds(pl.multiple_of(start, BLOCK), size), :]
                t_copies.append(pltpu.make_async_copy(ins[at], dst, in_sems.at[i]))
                at += 1
        first = len(items[0][0])
        for copy in t_copies[:first] + w_copies + t_copies[first:]:
            copy.start()
        pltpu.make_async_copy(w_ref, w_ref, w_sem).wait()
        done = []
        for i, (low, size, col) in enumerate(spans):
            pltpu.make_async_copy(t_ref.at[i], t_ref.at[i], in_sems.at[i]).wait()
            lanes = pl.ds(col, size)

            def step(j, carry):
                mine = pl.ds(pl.multiple_of(j * part, part), part)
                o_ref[mine, lanes] = nt_dot(t_ref[i, mine, :], w_ref[pl.ds(low, size), :]).astype(jnp.bfloat16)
                return carry

            lax.fori_loop(0, rows // part, step, 0)

            def rows_of(shift, low, size):
                start = (y + shift) % NY * BLOCK + low
                return o_ref.at[pl.ds(pl.multiple_of(start, half), size), lanes]

            pairs = [(o_ref.at[:, lanes], outs[0].at[:, lanes])] if direct else [
                (rows_of(2, 0, half), outs[1].at[:half, lanes]),
                (rows_of(1, half, half), outs[1].at[half:, lanes]),
                (rows_of(3, 0, half), outs[2].at[:half, lanes]),
                (rows_of(2, half, half), outs[2].at[half:, lanes]),
                (rows_of(1, 0, half), outs[3].at[:, lanes]),
                (rows_of(3, half, half), outs[4].at[:, lanes]),
                (rows_of(0, 0, BLOCK), outs[0].at[:, lanes]),
            ]
            for k, (src, dst) in enumerate(pairs):
                done.append(pltpu.make_async_copy(src, dst, out_sems.at[i, k]))
                done[-1].start()
        for copy in done:
            copy.wait()

    def out(m):
        return jax.ShapeDtypeStruct((m, n), jnp.bfloat16)

    return pl.pallas_call(
        kernel,
        in_specs=[hbm()] * (len(flat) + len(weights)),
        out_specs=[hbm()] * (1 if direct else 5),
        out_shape=[out(rows)] if direct else [out(BLOCK)] * 3 + [out(half)] * 2,
        scratch_shapes=[
            pltpu.VMEM((len(items), rows, width), jnp.bfloat16),
            pltpu.VMEM((total, width), jnp.bfloat16),
            pltpu.VMEM((rows, n), jnp.bfloat16),
            pltpu.SemaphoreType.DMA((len(items),)),
            pltpu.SemaphoreType.DMA,
            pltpu.SemaphoreType.DMA((len(items), 7)),
        ],
        cost_estimate=pl.CostEstimate(
            flops=2 * rows * width * n,
            bytes_accessed=2 * (len(items) * rows * width + width * total + rows * n),
            transcendentals=0,
        ),
        compiler_params=params(),
        name="partial_products",
    )(*flat, *weights)


def wide(a):
    return a.astype(jnp.float32)


def summed_on_arrival(parts):
    (product,) = parts
    blocks = product.reshape(NY, BLOCK, -1)
    blocks = lax.all_to_all(blocks, "gy", 0, 0, tiled=True)
    return jnp.sum(wide(blocks), axis=0).astype(jnp.bfloat16)


def step_one(parts):
    _, plus, minus, _, _ = parts
    from_minus = along_y(plus, 1)
    return from_minus, along_y(minus, -1)


def step_two(parts, first):
    half = BLOCK // 2
    _, _, _, plus, minus = parts
    from_minus, from_plus = first
    to_plus = (wide(plus) + wide(from_minus[:half])).astype(jnp.bfloat16)
    to_minus = (wide(minus) + wide(from_plus[half:])).astype(jnp.bfloat16)
    a = along_y(to_plus, 1)
    return a, along_y(to_minus, -1)


def summed(parts, first, second):
    half = BLOCK // 2
    own = parts[0]
    from_minus, from_plus = first
    low = wide(own[:half]) + wide(from_plus[:half]) + wide(second[0])
    high = wide(own[half:]) + wide(from_minus[half:]) + wide(second[1])
    return jnp.concatenate([low, high], axis=0).astype(jnp.bfloat16)


def pick_adapters(index, catalogs, shrinks):
    per, rank, n = catalogs[0].shape[1:]

    def kernel(index_ref, *refs):
        sources, terms, outs, sems = refs[:NX], refs[NX : NX + NY], refs[NX + NY : NX + 2 * NY], refs[NX + 2 * NY]
        for b in range(NY):
            pltpu.make_async_copy(terms[b], outs[b].at[:, n:], sems.at[NY + b]).start()
        x = lax.axis_index("gx") % NX
        zl = lax.axis_index("gx") // NX
        y = lax.axis_index("gy")
        for b in range(NY):
            a = index_ref[(y + b) % NY]
            owner = a // per
            rx = (owner % NX - x + NX) % NX
            rz = (owner // NX - zl + ZL) % ZL
            for k in range(NX):

                @pl.when(rx == k)
                def _():
                    pltpu.make_async_copy(sources[k].at[rz, a % per], outs[b].at[:, :n], sems.at[b]).start()

        for b in range(NY):
            pltpu.make_async_copy(sources[0].at[0, 0], outs[b].at[:, :n], sems.at[b]).wait()
            pltpu.make_async_copy(terms[b], outs[b].at[:, n:], sems.at[NY + b]).wait()

    return pl.pallas_call(
        kernel,
        in_specs=[smem()] + [hbm()] * (NX + NY),
        out_specs=[hbm()] * NY,
        out_shape=[jax.ShapeDtypeStruct((rank, n + shrinks[0].shape[1]), jnp.bfloat16)] * NY,
        scratch_shapes=[pltpu.SemaphoreType.DMA((2 * NY,))],
        compiler_params=params(),
        name="pick_adapters",
    )(index, *catalogs, *shrinks)


def finish(live, ups, pieces):
    rank = ups[0].shape[0]
    n = ups[0].shape[1] - TERMS * BLOCK
    flat = [a for parts in pieces for a in parts]

    def kernel(live_ref, *refs):
        up_refs, ins, out_ref, up_ref = refs[:NY], list(refs[NY:-2]), refs[-2], refs[-1]
        y = lax.axis_index("gy")
        zl = lax.axis_index("gx") // NX
        c = lax.axis_index("gz") % NC
        total = jnp.zeros((rank, BLOCK), jnp.float32)
        for k in range(NY):
            for term in range(TERMS):
                total = total + wide(up_refs[k][:, n + term * BLOCK : n + (term + 1) * BLOCK])
            up_ref[(y - k + NY) % NY] = up_refs[k][:, :n]
        low = total.astype(jnp.bfloat16)
        mask = lax.broadcasted_iota(jnp.int32, (BLOCK, n), 0) < live_ref[y]
        cols = [zl, (zl + 1 + 2 * c) % ZL, (zl + 3 - 2 * c) % ZL, (zl + 2) % ZL]
        for col, parts in zip(cols, pieces):
            refs_here = [ins.pop(0) for _ in parts]
            halves = [(refs_here[0], 0, FIRST)]
            halves.append((refs_here[-1], 0 if len(parts) == 2 else NX * FIRST, n // NX - FIRST))
            expand = lax.dot_general(
                low, up_ref[col], (((0,), (0,)), ((), ())), preferred_element_type=jnp.float32
            )
            blocks = [
                ref[:, base + x * size : base + (x + 1) * size] for x in range(NX) for ref, base, size in halves
            ]
            value = wide(jnp.concatenate(blocks, axis=1)) + 2.0 * expand
            out_ref[:, pl.ds(pl.multiple_of(col * n, 128), n)] = jnp.where(mask, value, 0.0).astype(jnp.bfloat16)

    vmem = pl.BlockSpec(memory_space=pltpu.VMEM)
    return pl.pallas_call(
        kernel,
        in_specs=[smem()] + [vmem] * (NY + len(flat)),
        out_specs=vmem,
        out_shape=jax.ShapeDtypeStruct((BLOCK, n * ZL), jnp.bfloat16),
        scratch_shapes=[pltpu.VMEM((NY, rank, n), jnp.bfloat16)],
        compiler_params=params(),
        name="finish",
    )(live, *ups, *flat)


FIRST = 128


def layer(tokens, base_up_weight, adapter_down_weight, adapter_up_weight, block_adapter_index, request_rows):
    rows, _ = tokens.shape
    y = lax.axis_index("gy")
    c = lax.axis_index("gz") % NC

    near = send(tokens, lambda z, x, c: ((z + 1 - 2 * c) % NZ, x, c))
    weights = []
    for part in (base_up_weight[:, :FIRST], base_up_weight[:, FIRST:]):
        pieces = [part.T]
        for r in range(1, NX):
            pieces.append(along_x(pieces[0], -r))
        weights.append(pieces)
    half = lax.dynamic_slice_in_dim(tokens, c * (rows // NC), rows // NC, 0)
    far = send(half, lambda z, x, c: ((z + 2 - 4 * c) % NZ, x, c))
    n = NX * base_up_weight.shape[1]
    up_z = [lax.dynamic_slice_in_dim(adapter_up_weight, y * n, n, 2)]
    for r in range(1, ZL):
        up_z.append(send(up_z[0], lambda z, x, c, r=r: (within(z, -r), x, c)))
    other = swap_cores(near)
    far_other = swap_cores(far)

    cut, rest = NX * FIRST, n - NX * FIRST
    a = partial_products([((near,), 0, 1), ((tokens,), 0, 1), ((other,), 0, 1)], weights[:1], direct=True)
    b = partial_products([((near,), 1, 2), ((far, far_other), 0, 2)], weights)
    b1 = step_one(b)
    d = partial_products([((tokens,), 0, 1), ((other,), 0, 1)], weights[1:], direct=True)
    b2 = step_two(b, b1)
    sum_a = summed_on_arrival(a)
    sum_b = summed(b, b1, b2)
    sum_d = summed_on_arrival(d)
    own0, own1 = sum_a[:, cut : 2 * cut], sum_d[:, :rest]

    def to_near(z, x, c):
        return within(z, 2 * c - 1), x, c

    def to_other(z, x, c):
        return within(z, 1 - 2 * c), x, c

    near0 = send(sum_a[:, :cut], to_near)
    other0 = send(sum_a[:, 2 * cut :], to_other)
    far = send(sum_b[:, rest:], lambda z, x, c: (within(z, 2), x, c))
    near1 = send(sum_b[:, :rest], to_near)
    other1 = send(sum_d[:, rest:], to_other)

    shrinks = shrink(tokens, adapter_down_weight, block_adapter_index)
    up_z = jnp.stack(up_z)
    catalogs = [up_z]
    for r in range(1, NX):
        catalogs.append(along_x(up_z, -r))
    ups = list(pick_adapters(block_adapter_index, catalogs, shrinks))
    for k in range(1, NY):
        ups[k] = along_y(ups[k], k)
    return finish(request_rows, ups, ((own0, own1), (near0, near1), (other0, other1), (far,)))


def solution(mesh):
    in_specs = (
        P("gx", "gy"),
        P("gy", ("gz", "gx")),
        P(None, None, "gy"),
        P("gx", None, "gz"),
        P("gx"),
        P("gx"),
    )
    out_specs = P(("gx", "gy"), "gz")
    return jax.shard_map(layer, mesh=mesh, in_specs=in_specs, out_specs=out_specs, check_vma=False)
```

```python
import jax
import jax.numpy as jnp
from jax import lax
from jax.experimental import pallas as pl
from jax.experimental.pallas import tpu as pltpu
from jax.sharding import PartitionSpec as P


BLOCK = 128
ZL, NX, NY, ZH, NC = 4, 4, 4, 2, 2
TERMS = 3
NZ = ZL * ZH
VMEM_LIMIT = 48 * 2**20


def device_perm(move):
    def place(z, x, c):
        return (z % ZL * NX + x) * ZH * NC + z // ZL * NC + c

    return [(place(z, x, c), place(*move(z, x, c))) for z in range(NZ) for x in range(NX) for c in range(NC)]


def send(a, move):
    return lax.ppermute(a, ("gx", "gz"), device_perm(move))


def within(z, shift):
    return z // ZL * ZL + (z + shift) % ZL


def along_x(a, shift):
    return lax.ppermute(a, "gx", [(z * NX + x, z * NX + (x + shift) % NX) for z in range(ZL) for x in range(NX)])


def along_y(a, shift):
    return lax.ppermute(a, "gy", [(y, (y + shift) % NY) for y in range(NY)])


def swap_cores(a):
    return send(a, lambda z, x, c: (z, x, 1 - c))


def nt_dot(a, b):
    return lax.dot_general(a, b, (((1,), (1,)), ((), ())), preferred_element_type=jnp.float32)


def hbm():
    return pl.BlockSpec(memory_space=pltpu.HBM)


def smem():
    return pl.BlockSpec(memory_space=pltpu.SMEM)


def params():
    return pltpu.CompilerParams(vmem_limit_bytes=VMEM_LIMIT)


def shrink(tokens, down, index):
    rank, width = down.shape[1:]

    def kernel(index_ref, tok_hbm, down_hbm, *refs):
        outs, (tok_ref, down_ref, out_ref, sems) = refs[:NY], refs[NY:]
        y = lax.axis_index("gy")
        loads = [pltpu.make_async_copy(tok_hbm, tok_ref, sems.at[0])]
        for b in range(NY):
            loads.append(pltpu.make_async_copy(down_hbm.at[index_ref[b]], down_ref.at[b], sems.at[1 + b]))
        for copy in loads:
            copy.start()
        for copy in loads:
            copy.wait()
        for b in range(NY):
            rest = nt_dot(down_ref[b], tok_ref[pl.ds(b * BLOCK, BLOCK), :])
            for term in range(TERMS):
                part = rest.astype(jnp.bfloat16)
                out_ref[b, :, term * BLOCK : (term + 1) * BLOCK] = part
                rest = rest - part.astype(jnp.float32)
        stores = [
            pltpu.make_async_copy(out_ref.at[(y + k) % NY], outs[k], sems.at[k]) for k in range(NY)
        ]
        for copy in stores:
            copy.start()
        for copy in stores:
            copy.wait()

    return pl.pallas_call(
        kernel,
        in_specs=[smem(), hbm(), hbm()],
        out_specs=[hbm()] * NY,
        out_shape=[jax.ShapeDtypeStruct((rank, TERMS * BLOCK), jnp.bfloat16)] * NY,
        scratch_shapes=[
            pltpu.VMEM(tokens.shape, jnp.bfloat16),
            pltpu.VMEM((NY, rank, width), jnp.bfloat16),
            pltpu.VMEM((NY, rank, TERMS * BLOCK), jnp.bfloat16),
            pltpu.SemaphoreType.DMA((1 + NY,)),
        ],
        compiler_params=params(),
        name="shrink",
    )(index, tokens, down)


def partial_products(items, weight_sets, direct=False):
    weights = [w for pieces in weight_sets for w in pieces]
    width = weights[0].shape[1]
    set_rows = [NX * pieces[0].shape[0] for pieces in weight_sets]
    total = sum(set_rows)
    rows = NY * BLOCK
    flat = [a for arrays, _, _ in items for a in arrays]
    spans, n = [], 0
    for _, lo, hi in items:
        spans.append((sum(set_rows[:lo]), sum(set_rows[lo:hi]), n))
        n += spans[-1][1]
    half = BLOCK // 2
    part = rows // 2

    def kernel(*refs):
        ins, w_in = refs[: len(flat)], refs[len(flat) : len(flat) + len(weights)]
        outs = refs[len(flat) + len(weights) : -6]
        t_ref, w_ref, o_ref, in_sems, w_sems, out_sems = refs[-6:]
        x = lax.axis_index("gx") % NX
        y = lax.axis_index("gy")
        c = lax.axis_index("gz") % NC
        w_copies, base = [], 0
        for i, w in enumerate(weights):
            nb = w.shape[0]
            at = pl.multiple_of(base + (x + i % NX) % NX * nb, 32)
            w_copies.append(pltpu.make_async_copy(w_in[i], w_ref.at[pl.ds(at, nb), :], w_sems.at[i // NX]))
            if i % NX == NX - 1:
                base += NX * nb
        t_copies, at = [], 0
        for i, (arrays, _, _) in enumerate(items):
            for j, array in enumerate(arrays):
                size = array.shape[0]
                start = (j if len(arrays) == 1 else (c + j) % NC) * size
                dst = t_ref.at[i, pl.ds(pl.multiple_of(start, BLOCK), size), :]
                t_copies.append(pltpu.make_async_copy(ins[at], dst, in_sems.at[i]))
                at += 1
        first = len(items[0][0])
        lo, hi = items[0][1] * NX, items[0][2] * NX
        for copy in t_copies[:first] + w_copies[lo:hi] + w_copies[:lo] + w_copies[hi:] + t_copies[first:]:
            copy.start()
        done, there = [], set()
        for i, (low, size, col) in enumerate(spans):
            for k in range(items[i][1], items[i][2]):
                if k not in there:
                    here = w_ref.at[pl.ds(sum(set_rows[:k]), set_rows[k]), :]
                    pltpu.make_async_copy(here, here, w_sems.at[k]).wait()
                    there.add(k)
            pltpu.make_async_copy(t_ref.at[i], t_ref.at[i], in_sems.at[i]).wait()
            lanes = pl.ds(col, size)

            def step(j, carry):
                mine = pl.ds(pl.multiple_of(j * part, part), part)
                o_ref[mine, lanes] = nt_dot(t_ref[i, mine, :], w_ref[pl.ds(low, size), :]).astype(jnp.bfloat16)
                return carry

            lax.fori_loop(0, rows // part, step, 0)

            def rows_of(shift, low, size):
                start = (y + shift) % NY * BLOCK + low
                return o_ref.at[pl.ds(pl.multiple_of(start, half), size), lanes]

            whole = [(rows_of(shift, 0, BLOCK), out.at[:, lanes]) for shift, out in zip((0, 1, 3, 2), outs)]
            pairs = whole if direct else [
                (rows_of(2, 0, half), outs[1].at[:half, lanes]),
                (rows_of(1, half, half), outs[1].at[half:, lanes]),
                (rows_of(3, 0, half), outs[2].at[:half, lanes]),
                (rows_of(2, half, half), outs[2].at[half:, lanes]),
                (rows_of(1, 0, half), outs[3].at[:, lanes]),
                (rows_of(3, half, half), outs[4].at[:, lanes]),
                (rows_of(0, 0, BLOCK), outs[0].at[:, lanes]),
            ]
            for k, (src, dst) in enumerate(pairs):
                done.append(pltpu.make_async_copy(src, dst, out_sems.at[i, k]))
                done[-1].start()
        for copy in done:
            copy.wait()

    def out(m):
        return jax.ShapeDtypeStruct((m, n), jnp.bfloat16)

    return pl.pallas_call(
        kernel,
        in_specs=[hbm()] * (len(flat) + len(weights)),
        out_specs=[hbm()] * (4 if direct else 5),
        out_shape=[out(BLOCK)] * 4 if direct else [out(BLOCK)] * 3 + [out(half)] * 2,
        scratch_shapes=[
            pltpu.VMEM((len(items), rows, width), jnp.bfloat16),
            pltpu.VMEM((total, width), jnp.bfloat16),
            pltpu.VMEM((rows, n), jnp.bfloat16),
            pltpu.SemaphoreType.DMA((len(items),)),
            pltpu.SemaphoreType.DMA((len(weight_sets),)),
            pltpu.SemaphoreType.DMA((len(items), 7)),
        ],
        cost_estimate=pl.CostEstimate(
            flops=2 * rows * width * n,
            bytes_accessed=2 * (len(items) * rows * width + width * total + rows * n),
            transcendentals=0,
        ),
        compiler_params=params(),
        name="partial_products",
    )(*flat, *weights)


def wide(a):
    return a.astype(jnp.float32)


def summed_direct(parts):
    arrived = []
    for part, shift in zip(parts[1:], (1, -1, 2)):
        arrived.append(along_y(part, shift))
    total = wide(parts[0])
    for part in arrived:
        total = total + wide(part)
    return total.astype(jnp.bfloat16)


def step_one(parts):
    _, plus, minus, _, _ = parts
    from_minus = along_y(plus, 1)
    return from_minus, along_y(minus, -1)


def step_two(parts, first):
    half = BLOCK // 2
    _, _, _, plus, minus = parts
    from_minus, from_plus = first
    to_plus = (wide(plus) + wide(from_minus[:half])).astype(jnp.bfloat16)
    to_minus = (wide(minus) + wide(from_plus[half:])).astype(jnp.bfloat16)
    a = along_y(to_plus, 1)
    return a, along_y(to_minus, -1)


def summed(parts, first, second):
    half = BLOCK // 2
    own = parts[0]
    from_minus, from_plus = first
    low = wide(own[:half]) + wide(from_plus[:half]) + wide(second[0])
    high = wide(own[half:]) + wide(from_minus[half:]) + wide(second[1])
    return jnp.concatenate([low, high], axis=0).astype(jnp.bfloat16)


def pick_adapters(index, catalogs, shrinks):
    per, rank, n = catalogs[0].shape[1:]

    def kernel(index_ref, *refs):
        sources, terms, outs, sems = refs[:NX], refs[NX : NX + NY], refs[NX + NY : NX + 2 * NY], refs[NX + 2 * NY]
        for b in range(NY):
            pltpu.make_async_copy(terms[b], outs[b].at[:, n:], sems.at[NY + b]).start()
        x = lax.axis_index("gx") % NX
        zl = lax.axis_index("gx") // NX
        y = lax.axis_index("gy")
        for b in range(NY):
            a = index_ref[(y + b) % NY]
            owner = a // per
            rx = (owner % NX - x + NX) % NX
            rz = (owner // NX - zl + ZL) % ZL
            for k in range(NX):

                @pl.when(rx == k)
                def _():
                    pltpu.make_async_copy(sources[k].at[rz, a % per], outs[b].at[:, :n], sems.at[b]).start()

        for b in range(NY):
            pltpu.make_async_copy(sources[0].at[0, 0], outs[b].at[:, :n], sems.at[b]).wait()
            pltpu.make_async_copy(terms[b], outs[b].at[:, n:], sems.at[NY + b]).wait()

    return pl.pallas_call(
        kernel,
        in_specs=[smem()] + [hbm()] * (NX + NY),
        out_specs=[hbm()] * NY,
        out_shape=[jax.ShapeDtypeStruct((rank, n + shrinks[0].shape[1]), jnp.bfloat16)] * NY,
        scratch_shapes=[pltpu.SemaphoreType.DMA((2 * NY,))],
        compiler_params=params(),
        name="pick_adapters",
    )(index, *catalogs, *shrinks)


def finish(live, ups, pieces):
    rank = ups[0].shape[0]
    n = ups[0].shape[1] - TERMS * BLOCK
    flat = [a for parts in pieces for a in parts]

    def kernel(live_ref, *refs):
        up_refs, ins, out_ref, up_ref = refs[:NY], list(refs[NY:-2]), refs[-2], refs[-1]
        y = lax.axis_index("gy")
        zl = lax.axis_index("gx") // NX
        c = lax.axis_index("gz") % NC
        total = jnp.zeros((rank, BLOCK), jnp.float32)
        for k in range(NY):
            for term in range(TERMS):
                total = total + wide(up_refs[k][:, n + term * BLOCK : n + (term + 1) * BLOCK])
            up_ref[(y - k + NY) % NY] = up_refs[k][:, :n]
        low = total.astype(jnp.bfloat16)
        mask = lax.broadcasted_iota(jnp.int32, (BLOCK, n), 0) < live_ref[y]
        cols = [zl, (zl + 1 + 2 * c) % ZL, (zl + 3 - 2 * c) % ZL, (zl + 2) % ZL]
        for col, parts in zip(cols, pieces):
            refs_here = [ins.pop(0) for _ in parts]
            halves = [(refs_here[0], 0, FIRST)]
            halves.append((refs_here[-1], 0 if len(parts) == 2 else NX * FIRST, n // NX - FIRST))
            expand = lax.dot_general(
                low, up_ref[col], (((0,), (0,)), ((), ())), preferred_element_type=jnp.float32
            )
            blocks = [
                ref[:, base + x * size : base + (x + 1) * size] for x in range(NX) for ref, base, size in halves
            ]
            value = wide(jnp.concatenate(blocks, axis=1)) + 2.0 * expand
            out_ref[:, pl.ds(pl.multiple_of(col * n, 128), n)] = jnp.where(mask, value, 0.0).astype(jnp.bfloat16)

    vmem = pl.BlockSpec(memory_space=pltpu.VMEM)
    return pl.pallas_call(
        kernel,
        in_specs=[smem()] + [vmem] * (NY + len(flat)),
        out_specs=vmem,
        out_shape=jax.ShapeDtypeStruct((BLOCK, n * ZL), jnp.bfloat16),
        scratch_shapes=[pltpu.VMEM((NY, rank, n), jnp.bfloat16)],
        compiler_params=params(),
        name="finish",
    )(live, *ups, *flat)


FIRST = 160


def layer(tokens, base_up_weight, adapter_down_weight, adapter_up_weight, block_adapter_index, request_rows):
    rows, _ = tokens.shape
    y = lax.axis_index("gy")
    c = lax.axis_index("gz") % NC

    near = send(tokens, lambda z, x, c: ((z + 1 - 2 * c) % NZ, x, c))
    weights = []
    for part in (base_up_weight[:, :FIRST], base_up_weight[:, FIRST:]):
        pieces = [part.T]
        for r in range(1, NX):
            pieces.append(along_x(pieces[0], -r))
        weights.append(pieces)
    n = NX * base_up_weight.shape[1]
    up_z = [lax.dynamic_slice_in_dim(adapter_up_weight, y * n, n, 2)]
    for r in range(1, ZL):
        up_z.append(send(up_z[0], lambda z, x, c, r=r: (within(z, -r), x, c)))
    other = swap_cores(near)
    half = lax.dynamic_slice_in_dim(near, c * (rows // NC), rows // NC, 0)
    far = send(half, lambda z, x, c: ((z + 1 - 2 * c) % NZ, x, c))
    far_other = swap_cores(far)

    a = partial_products([((near,), 0, 1), ((other,), 0, 1)], weights[:1], direct=True)
    sum_a = summed_direct(a)
    b = partial_products([((near,), 1, 2), ((far, far_other), 0, 2)], weights)
    b1 = step_one(b)
    d = partial_products([((other,), 1, 2), ((tokens,), 0, 2)], weights)
    b2 = step_two(b, b1)
    d1 = step_one(d)
    cut, rest = NX * FIRST, n - NX * FIRST
    sum_b = summed(b, b1, b2)
    d2 = step_two(d, d1)
    sum_d = summed(d, d1, d2)

    def to_near(z, x, c):
        return within(z, 2 * c - 1), x, c

    def to_other(z, x, c):
        return within(z, 1 - 2 * c), x, c

    near0 = send(sum_a[:, :cut], to_near)
    other0 = send(sum_a[:, cut:], to_other)
    far = send(sum_b[:, rest:], lambda z, x, c: (within(z, 2), x, c))
    near1 = send(sum_b[:, :rest], to_near)
    other1 = send(sum_d[:, :rest], to_other)
    own = sum_d[:, rest:]

    shrinks = shrink(tokens, adapter_down_weight, block_adapter_index)
    up_z = jnp.stack(up_z)
    catalogs = [up_z]
    for r in range(1, NX):
        catalogs.append(along_x(up_z, -r))
    ups = list(pick_adapters(block_adapter_index, catalogs, shrinks))
    for k in range(1, NY):
        ups[k] = along_y(ups[k], k)
    return finish(request_rows, ups, ((own,), (near0, near1), (other0, other1), (far,)))


def solution(mesh):
    in_specs = (
        P("gx", "gy"),
        P("gy", ("gz", "gx")),
        P(None, None, "gy"),
        P("gx", None, "gz"),
        P("gx"),
        P("gx"),
    )
    out_specs = P(("gx", "gy"), "gz")
    return jax.shard_map(layer, mesh=mesh, in_specs=in_specs, out_specs=out_specs, check_vma=False)
```

```python
import jax
import jax.numpy as jnp
from jax import lax
from jax.experimental import pallas as pl
from jax.experimental.pallas import tpu as pltpu
from jax.sharding import PartitionSpec as P


BLOCK = 128
ZL, NX, NY, ZH, NC = 4, 4, 4, 2, 2
TERMS = 3
NZ = ZL * ZH
VMEM_LIMIT = 20 * 2**20


def device_perm(move):
    def place(z, x, c):
        return (z % ZL * NX + x) * ZH * NC + z // ZL * NC + c

    return [(place(z, x, c), place(*move(z, x, c))) for z in range(NZ) for x in range(NX) for c in range(NC)]


def send(a, move):
    return lax.ppermute(a, ("gx", "gz"), device_perm(move))


def within(z, shift):
    return z // ZL * ZL + (z + shift) % ZL


def along_x(a, shift):
    return lax.ppermute(a, "gx", [(z * NX + x, z * NX + (x + shift) % NX) for z in range(ZL) for x in range(NX)])


def along_y(a, shift):
    return lax.ppermute(a, "gy", [(y, (y + shift) % NY) for y in range(NY)])


def swap_cores(a):
    return send(a, lambda z, x, c: (z, x, 1 - c))


def nt_dot(a, b):
    return lax.dot_general(a, b, (((1,), (1,)), ((), ())), preferred_element_type=jnp.float32)


def hbm():
    return pl.BlockSpec(memory_space=pltpu.HBM)


def smem():
    return pl.BlockSpec(memory_space=pltpu.SMEM)


def params():
    return pltpu.CompilerParams(vmem_limit_bytes=VMEM_LIMIT)


def shrink(tokens, down, index):
    rank, width = down.shape[1:]

    def kernel(index_ref, tok_hbm, down_hbm, *refs):
        outs, (tok_ref, down_ref, out_ref, sems) = refs[:NY], refs[NY:]
        y = lax.axis_index("gy")
        loads = [pltpu.make_async_copy(tok_hbm, tok_ref, sems.at[0])]
        for b in range(NY):
            loads.append(pltpu.make_async_copy(down_hbm.at[index_ref[b]], down_ref.at[b], sems.at[1 + b]))
        for copy in loads:
            copy.start()
        for copy in loads:
            copy.wait()
        for b in range(NY):
            rest = nt_dot(down_ref[b], tok_ref[pl.ds(b * BLOCK, BLOCK), :])
            for term in range(TERMS):
                part = rest.astype(jnp.bfloat16)
                out_ref[b, :, term * BLOCK : (term + 1) * BLOCK] = part
                rest = rest - part.astype(jnp.float32)
        stores = [
            pltpu.make_async_copy(out_ref.at[(y + k) % NY], outs[k], sems.at[k]) for k in range(NY)
        ]
        for copy in stores:
            copy.start()
        for copy in stores:
            copy.wait()

    return pl.pallas_call(
        kernel,
        in_specs=[smem(), hbm(), hbm()],
        out_specs=[hbm()] * NY,
        out_shape=[jax.ShapeDtypeStruct((rank, TERMS * BLOCK), jnp.bfloat16)] * NY,
        scratch_shapes=[
            pltpu.VMEM(tokens.shape, jnp.bfloat16),
            pltpu.VMEM((NY, rank, width), jnp.bfloat16),
            pltpu.VMEM((NY, rank, TERMS * BLOCK), jnp.bfloat16),
            pltpu.SemaphoreType.DMA((1 + NY,)),
        ],
        compiler_params=params(),
        name="shrink",
    )(index, tokens, down)


def partial_products(items, weight_sets, direct=False):
    weights = [w for pieces in weight_sets for w in pieces]
    width = weights[0].shape[1]
    set_rows = [NX * pieces[0].shape[0] for pieces in weight_sets]
    total = sum(set_rows)
    rows = NY * BLOCK
    flat = [a for arrays, _, _ in items for a in arrays]
    spans, n = [], 0
    for _, lo, hi in items:
        spans.append((sum(set_rows[:lo]), sum(set_rows[lo:hi]), n))
        n += spans[-1][1]
    half = BLOCK // 2
    part = rows // 2

    def kernel(*refs):
        ins, w_in = refs[: len(flat)], refs[len(flat) : len(flat) + len(weights)]
        outs = refs[len(flat) + len(weights) : -6]
        t_ref, w_ref, o_ref, in_sems, w_sems, out_sems = refs[-6:]
        x = lax.axis_index("gx") % NX
        y = lax.axis_index("gy")
        c = lax.axis_index("gz") % NC
        w_copies, base = [], 0
        for i, w in enumerate(weights):
            nb = w.shape[0]
            at = pl.multiple_of(base + (x + i % NX) % NX * nb, 32)
            w_copies.append(pltpu.make_async_copy(w_in[i], w_ref.at[pl.ds(at, nb), :], w_sems.at[i // NX]))
            if i % NX == NX - 1:
                base += NX * nb
        t_copies, at = [], 0
        for i, (arrays, _, _) in enumerate(items):
            for j, array in enumerate(arrays):
                size = array.shape[0]
                start = (j if len(arrays) == 1 else (c + j) % NC) * size
                dst = t_ref.at[i, pl.ds(pl.multiple_of(start, BLOCK), size), :]
                t_copies.append(pltpu.make_async_copy(ins[at], dst, in_sems.at[i]))
                at += 1
        first = len(items[0][0])
        lo, hi = items[0][1] * NX, items[0][2] * NX
        for copy in t_copies[:first] + w_copies[lo:hi] + w_copies[:lo] + w_copies[hi:] + t_copies[first:]:
            copy.start()
        done, there = [], set()
        for i, (low, size, col) in enumerate(spans):
            for k in range(items[i][1], items[i][2]):
                if k not in there:
                    here = w_ref.at[pl.ds(sum(set_rows[:k]), set_rows[k]), :]
                    pltpu.make_async_copy(here, here, w_sems.at[k]).wait()
                    there.add(k)
            pltpu.make_async_copy(t_ref.at[i], t_ref.at[i], in_sems.at[i]).wait()
            lanes = pl.ds(col, size)

            def step(j, carry):
                mine = pl.ds(pl.multiple_of(j * part, part), part)
                o_ref[mine, lanes] = nt_dot(t_ref[i, mine, :], w_ref[pl.ds(low, size), :]).astype(jnp.bfloat16)
                return carry

            lax.fori_loop(0, rows // part, step, 0)

            def rows_of(shift, low, size):
                start = (y + shift) % NY * BLOCK + low
                return o_ref.at[pl.ds(pl.multiple_of(start, half), size), lanes]

            whole = [(rows_of(shift, 0, BLOCK), out.at[:, lanes]) for shift, out in zip((0, 1, 3, 2), outs)]
            pairs = whole if direct else [
                (rows_of(2, 0, half), outs[1].at[:half, lanes]),
                (rows_of(1, half, half), outs[1].at[half:, lanes]),
                (rows_of(3, 0, half), outs[2].at[:half, lanes]),
                (rows_of(2, half, half), outs[2].at[half:, lanes]),
                (rows_of(1, 0, half), outs[3].at[:, lanes]),
                (rows_of(3, half, half), outs[4].at[:, lanes]),
                (rows_of(0, 0, BLOCK), outs[0].at[:, lanes]),
            ]
            for k, (src, dst) in enumerate(pairs):
                done.append(pltpu.make_async_copy(src, dst, out_sems.at[i, k]))
                done[-1].start()
        for copy in done:
            copy.wait()

    def out(m):
        return jax.ShapeDtypeStruct((m, n), jnp.bfloat16)

    return pl.pallas_call(
        kernel,
        in_specs=[hbm()] * (len(flat) + len(weights)),
        out_specs=[hbm()] * (4 if direct else 5),
        out_shape=[out(BLOCK)] * 4 if direct else [out(BLOCK)] * 3 + [out(half)] * 2,
        scratch_shapes=[
            pltpu.VMEM((len(items), rows, width), jnp.bfloat16),
            pltpu.VMEM((total, width), jnp.bfloat16),
            pltpu.VMEM((rows, n), jnp.bfloat16),
            pltpu.SemaphoreType.DMA((len(items),)),
            pltpu.SemaphoreType.DMA((len(weight_sets),)),
            pltpu.SemaphoreType.DMA((len(items), 7)),
        ],
        cost_estimate=pl.CostEstimate(
            flops=2 * rows * width * n,
            bytes_accessed=2 * (len(items) * rows * width + width * total + rows * n),
            transcendentals=0,
        ),
        compiler_params=params(),
        name="partial_products",
    )(*flat, *weights)


def wide(a):
    return a.astype(jnp.float32)


def summed_direct(parts):
    arrived = []
    for part, shift in zip(parts[1:], (1, -1, 2)):
        arrived.append(along_y(part, shift))
    total = wide(parts[0])
    for part in arrived:
        total = total + wide(part)
    return total.astype(jnp.bfloat16)


def step_one(parts):
    _, plus, minus, _, _ = parts
    from_minus = along_y(plus, 1)
    return from_minus, along_y(minus, -1)


def step_two(parts, first):
    half = BLOCK // 2
    _, _, _, plus, minus = parts
    from_minus, from_plus = first
    to_plus = (wide(plus) + wide(from_minus[:half])).astype(jnp.bfloat16)
    to_minus = (wide(minus) + wide(from_plus[half:])).astype(jnp.bfloat16)
    a = along_y(to_plus, 1)
    return a, along_y(to_minus, -1)


def summed(parts, first, second):
    half = BLOCK // 2
    own = parts[0]
    from_minus, from_plus = first
    low = wide(own[:half]) + wide(from_plus[:half]) + wide(second[0])
    high = wide(own[half:]) + wide(from_minus[half:]) + wide(second[1])
    return jnp.concatenate([low, high], axis=0).astype(jnp.bfloat16)


def pick_adapters(index, catalogs, shrinks):
    per, rank, n = catalogs[0].shape[1:]

    def kernel(index_ref, *refs):
        sources, terms, outs, sems = refs[:NX], refs[NX : NX + NY], refs[NX + NY : NX + 2 * NY], refs[NX + 2 * NY]
        for b in range(NY):
            pltpu.make_async_copy(terms[b], outs[b].at[:, n:], sems.at[NY + b]).start()
        x = lax.axis_index("gx") % NX
        zl = lax.axis_index("gx") // NX
        y = lax.axis_index("gy")
        for b in range(NY):
            a = index_ref[(y + b) % NY]
            owner = a // per
            rx = (owner % NX - x + NX) % NX
            rz = (owner // NX - zl + ZL) % ZL
            for k in range(NX):

                @pl.when(rx == k)
                def _():
                    pltpu.make_async_copy(sources[k].at[rz, a % per], outs[b].at[:, :n], sems.at[b]).start()

        for b in range(NY):
            pltpu.make_async_copy(sources[0].at[0, 0], outs[b].at[:, :n], sems.at[b]).wait()
            pltpu.make_async_copy(terms[b], outs[b].at[:, n:], sems.at[NY + b]).wait()

    return pl.pallas_call(
        kernel,
        in_specs=[smem()] + [hbm()] * (NX + NY),
        out_specs=[hbm()] * NY,
        out_shape=[jax.ShapeDtypeStruct((rank, n + shrinks[0].shape[1]), jnp.bfloat16)] * NY,
        scratch_shapes=[pltpu.SemaphoreType.DMA((2 * NY,))],
        compiler_params=params(),
        name="pick_adapters",
    )(index, *catalogs, *shrinks)


def finish(live, ups, places, pieces, before=()):
    rank = ups[0].shape[0]
    n = ups[0].shape[1] - TERMS * BLOCK
    flat = [a for parts in pieces for a in parts]

    def kernel(live_ref, *refs):
        refs = refs[len(before) :]
        up_refs, ins = refs[:NY], list(refs[NY : NY + len(flat)])
        out_hbm, up_ref, out_ref, sems = refs[NY + len(flat) :]
        y = lax.axis_index("gy")
        zl = lax.axis_index("gx") // NX
        c = lax.axis_index("gz") % NC
        total = jnp.zeros((rank, BLOCK), jnp.float32)
        for k in range(NY):
            for term in range(TERMS):
                total = total + wide(up_refs[k][:, n + term * BLOCK : n + (term + 1) * BLOCK])
            up_ref[(y - k + NY) % NY] = up_refs[k][:, :n]
        low = total.astype(jnp.bfloat16)
        mask = lax.broadcasted_iota(jnp.int32, (BLOCK, n), 0) < live_ref[y]
        copies = []
        for i, (place, parts) in enumerate(zip(places, pieces)):
            col = (zl + place[0] + (place[1] - place[0]) * c) % ZL
            refs_here = [ins.pop(0) for _ in parts]
            halves = [(refs_here[0], 0, FIRST)]
            halves.append((refs_here[-1], 0 if len(parts) == 2 else NX * FIRST, n // NX - FIRST))
            expand = lax.dot_general(
                low, up_ref[col], (((0,), (0,)), ((), ())), preferred_element_type=jnp.float32
            )
            blocks = [
                ref[:, base + x * size : base + (x + 1) * size] for x in range(NX) for ref, base, size in halves
            ]
            value = wide(jnp.concatenate(blocks, axis=1)) + 2.0 * expand
            out_ref[i] = jnp.where(mask, value, 0.0).astype(jnp.bfloat16)
            there = out_hbm.at[:, pl.ds(pl.multiple_of(col * n, 128), n)]
            copies.append(pltpu.make_async_copy(out_ref.at[i], there, sems.at[i]))
            copies[-1].start()
        for copy in copies:
            copy.wait()

    vmem = pl.BlockSpec(memory_space=pltpu.VMEM)
    return pl.pallas_call(
        kernel,
        in_specs=[smem()] + [hbm()] * len(before) + [vmem] * (NY + len(flat)),
        out_specs=hbm(),
        out_shape=jax.ShapeDtypeStruct((BLOCK, n * ZL), jnp.bfloat16),
        scratch_shapes=[
            pltpu.VMEM((NY, rank, n), jnp.bfloat16),
            pltpu.VMEM((len(pieces), BLOCK, n), jnp.bfloat16),
            pltpu.SemaphoreType.DMA((len(pieces),)),
        ],
        input_output_aliases={1: 0} if before else {},
        compiler_params=params(),
        name="finish",
    )(live, *before, *ups, *flat)


FIRST = 128


def layer(tokens, base_up_weight, adapter_down_weight, adapter_up_weight, block_adapter_index, request_rows):
    rows, _ = tokens.shape
    y = lax.axis_index("gy")
    c = lax.axis_index("gz") % NC

    near = send(tokens, lambda z, x, c: ((z + 1 - 2 * c) % NZ, x, c))
    weights = []
    for part in (base_up_weight[:, :FIRST], base_up_weight[:, FIRST:]):
        pieces = [part.T]
        for r in range(1, NX):
            pieces.append(along_x(pieces[0], -r))
        weights.append(pieces)
    n = NX * base_up_weight.shape[1]
    up_z = [lax.dynamic_slice_in_dim(adapter_up_weight, y * n, n, 2)]
    for r in range(1, ZL):
        up_z.append(send(up_z[0], lambda z, x, c, r=r: (within(z, -r), x, c)))
    other = swap_cores(near)
    half = lax.dynamic_slice_in_dim(near, c * (rows // NC), rows // NC, 0)
    far = send(half, lambda z, x, c: ((z + 1 - 2 * c) % NZ, x, c))
    far_other = swap_cores(far)

    a = partial_products([((near,), 0, 1), ((other,), 0, 1)], weights[:1], direct=True)
    sum_a = summed_direct(a)
    b = partial_products([((near,), 1, 2), ((far, far_other), 0, 2)], weights, direct=True)
    sum_b = summed_direct(b)
    d = partial_products([((other,), 1, 2), ((tokens,), 0, 2)], weights)
    d1 = step_one(d)
    cut, rest = NX * FIRST, n - NX * FIRST
    d2 = step_two(d, d1)
    sum_d = summed(d, d1, d2)

    def to_near(z, x, c):
        return within(z, 2 * c - 1), x, c

    def to_other(z, x, c):
        return within(z, 1 - 2 * c), x, c

    near0 = send(sum_a[:, :cut], to_near)
    other0 = send(sum_a[:, cut:], to_other)
    far = send(sum_b[:, rest:], lambda z, x, c: (within(z, 2), x, c))
    near1 = send(sum_b[:, :rest], to_near)
    other1 = send(sum_d[:, :rest], to_other)
    own = sum_d[:, rest:]

    shrinks = shrink(tokens, adapter_down_weight, block_adapter_index)
    up_z = jnp.stack(up_z)
    catalogs = [up_z]
    for r in range(1, NX):
        catalogs.append(along_x(up_z, -r))
    ups = list(pick_adapters(block_adapter_index, catalogs, shrinks))
    for k in range(1, NY):
        ups[k] = along_y(ups[k], k)
    ready = finish(request_rows, ups, ((0, 0), (1, 3), (2, 2)), ((own,), (near0, near1), (far,)))
    return finish(request_rows, ups, ((3, 1),), ((other0, other1),), (ready,))


def solution(mesh):
    in_specs = (
        P("gx", "gy"),
        P("gy", ("gz", "gx")),
        P(None, None, "gy"),
        P("gx", None, "gz"),
        P("gx"),
        P("gx"),
    )
    out_specs = P(("gx", "gy"), "gz")
    return jax.shard_map(layer, mesh=mesh, in_specs=in_specs, out_specs=out_specs, check_vma=False)
```

```python
import jax
import jax.numpy as jnp
from jax import lax
from jax.experimental import pallas as pl
from jax.experimental.pallas import tpu as pltpu
from jax.sharding import PartitionSpec as P


BLOCK = 128
ZL, NX, NY, ZH, NC = 4, 4, 4, 2, 2
TERMS = 3
NZ = ZL * ZH
VMEM_LIMIT = 20 * 2**20


def device_perm(move):
    def place(z, x, c):
        return (z % ZL * NX + x) * ZH * NC + z // ZL * NC + c

    return [(place(z, x, c), place(*move(z, x, c))) for z in range(NZ) for x in range(NX) for c in range(NC)]


def send(a, move):
    return lax.ppermute(a, ("gx", "gz"), device_perm(move))


def within(z, shift):
    return z // ZL * ZL + (z + shift) % ZL


def along_x(a, shift):
    return lax.ppermute(a, "gx", [(z * NX + x, z * NX + (x + shift) % NX) for z in range(ZL) for x in range(NX)])


def along_y(a, shift):
    return lax.ppermute(a, "gy", [(y, (y + shift) % NY) for y in range(NY)])


def swap_cores(a):
    return send(a, lambda z, x, c: (z, x, 1 - c))


def nt_dot(a, b):
    return lax.dot_general(a, b, (((1,), (1,)), ((), ())), preferred_element_type=jnp.float32)


def hbm():
    return pl.BlockSpec(memory_space=pltpu.HBM)


def smem():
    return pl.BlockSpec(memory_space=pltpu.SMEM)


def params():
    return pltpu.CompilerParams(vmem_limit_bytes=VMEM_LIMIT)


def shrink(tokens, down, index):
    rank, width = down.shape[1:]

    def kernel(index_ref, tok_hbm, down_hbm, *refs):
        outs, (tok_ref, down_ref, out_ref, sems) = refs[:NY], refs[NY:]
        y = lax.axis_index("gy")
        loads = [pltpu.make_async_copy(tok_hbm, tok_ref, sems.at[0])]
        for b in range(NY):
            loads.append(pltpu.make_async_copy(down_hbm.at[index_ref[b]], down_ref.at[b], sems.at[1 + b]))
        for copy in loads:
            copy.start()
        for copy in loads:
            copy.wait()
        for b in range(NY):
            rest = nt_dot(down_ref[b], tok_ref[pl.ds(b * BLOCK, BLOCK), :])
            for term in range(TERMS):
                part = rest.astype(jnp.bfloat16)
                out_ref[b, :, term * BLOCK : (term + 1) * BLOCK] = part
                rest = rest - part.astype(jnp.float32)
        stores = [
            pltpu.make_async_copy(out_ref.at[(y + k) % NY], outs[k], sems.at[k]) for k in range(NY)
        ]
        for copy in stores:
            copy.start()
        for copy in stores:
            copy.wait()

    return pl.pallas_call(
        kernel,
        in_specs=[smem(), hbm(), hbm()],
        out_specs=[hbm()] * NY,
        out_shape=[jax.ShapeDtypeStruct((rank, TERMS * BLOCK), jnp.bfloat16)] * NY,
        scratch_shapes=[
            pltpu.VMEM(tokens.shape, jnp.bfloat16),
            pltpu.VMEM((NY, rank, width), jnp.bfloat16),
            pltpu.VMEM((NY, rank, TERMS * BLOCK), jnp.bfloat16),
            pltpu.SemaphoreType.DMA((1 + NY,)),
        ],
        compiler_params=params(),
        name="shrink",
    )(index, tokens, down)


def partial_products(items, weight_sets, direct=False):
    weights = [w for pieces in weight_sets for w in pieces]
    width = weights[0].shape[1]
    set_rows = [NX * pieces[0].shape[0] for pieces in weight_sets]
    total = sum(set_rows)
    rows = NY * BLOCK
    flat = [a for arrays, _, _ in items for a in arrays]
    spans, n = [], 0
    for _, lo, hi in items:
        spans.append((sum(set_rows[:lo]), sum(set_rows[lo:hi]), n))
        n += spans[-1][1]
    half = BLOCK // 2
    part = rows // 2

    def kernel(*refs):
        ins, w_in = refs[: len(flat)], refs[len(flat) : len(flat) + len(weights)]
        outs = refs[len(flat) + len(weights) : -6]
        t_ref, w_ref, o_ref, in_sems, w_sems, out_sems = refs[-6:]
        x = lax.axis_index("gx") % NX
        y = lax.axis_index("gy")
        c = lax.axis_index("gz") % NC
        w_copies, base = [], 0
        for i, w in enumerate(weights):
            nb = w.shape[0]
            at = pl.multiple_of(base + (x + i % NX) % NX * nb, 32)
            w_copies.append(pltpu.make_async_copy(w_in[i], w_ref.at[pl.ds(at, nb), :], w_sems.at[i // NX]))
            if i % NX == NX - 1:
                base += NX * nb
        t_copies, at = [], 0
        for i, (arrays, _, _) in enumerate(items):
            for j, array in enumerate(arrays):
                size = array.shape[0]
                start = (j if len(arrays) == 1 else (c + j) % NC) * size
                dst = t_ref.at[i, pl.ds(pl.multiple_of(start, BLOCK), size), :]
                t_copies.append(pltpu.make_async_copy(ins[at], dst, in_sems.at[i]))
                at += 1
        first = len(items[0][0])
        lo, hi = items[0][1] * NX, items[0][2] * NX
        for copy in t_copies[:first] + w_copies[lo:hi] + w_copies[:lo] + w_copies[hi:] + t_copies[first:]:
            copy.start()
        done, there = [], set()
        for i, (low, size, col) in enumerate(spans):
            for k in range(items[i][1], items[i][2]):
                if k not in there:
                    here = w_ref.at[pl.ds(sum(set_rows[:k]), set_rows[k]), :]
                    pltpu.make_async_copy(here, here, w_sems.at[k]).wait()
                    there.add(k)
            pltpu.make_async_copy(t_ref.at[i], t_ref.at[i], in_sems.at[i]).wait()
            lanes = pl.ds(col, size)

            def step(j, carry):
                mine = pl.ds(pl.multiple_of(j * part, part), part)
                o_ref[mine, lanes] = nt_dot(t_ref[i, mine, :], w_ref[pl.ds(low, size), :]).astype(jnp.bfloat16)
                return carry

            lax.fori_loop(0, rows // part, step, 0)

            def rows_of(shift, low, size):
                start = (y + shift) % NY * BLOCK + low
                return o_ref.at[pl.ds(pl.multiple_of(start, half), size), lanes]

            whole = [(rows_of(shift, 0, BLOCK), out.at[:, lanes]) for shift, out in zip((0, 1, 3, 2), outs)]
            pairs = whole if direct else [
                (rows_of(2, 0, half), outs[1].at[:half, lanes]),
                (rows_of(1, half, half), outs[1].at[half:, lanes]),
                (rows_of(3, 0, half), outs[2].at[:half, lanes]),
                (rows_of(2, half, half), outs[2].at[half:, lanes]),
                (rows_of(1, 0, half), outs[3].at[:, lanes]),
                (rows_of(3, half, half), outs[4].at[:, lanes]),
                (rows_of(0, 0, BLOCK), outs[0].at[:, lanes]),
            ]
            for k, (src, dst) in enumerate(pairs):
                done.append(pltpu.make_async_copy(src, dst, out_sems.at[i, k]))
                done[-1].start()
        for copy in done:
            copy.wait()

    def out(m):
        return jax.ShapeDtypeStruct((m, n), jnp.bfloat16)

    return pl.pallas_call(
        kernel,
        in_specs=[hbm()] * (len(flat) + len(weights)),
        out_specs=[hbm()] * (4 if direct else 5),
        out_shape=[out(BLOCK)] * 4 if direct else [out(BLOCK)] * 3 + [out(half)] * 2,
        scratch_shapes=[
            pltpu.VMEM((len(items), rows, width), jnp.bfloat16),
            pltpu.VMEM((total, width), jnp.bfloat16),
            pltpu.VMEM((rows, n), jnp.bfloat16),
            pltpu.SemaphoreType.DMA((len(items),)),
            pltpu.SemaphoreType.DMA((len(weight_sets),)),
            pltpu.SemaphoreType.DMA((len(items), 7)),
        ],
        cost_estimate=pl.CostEstimate(
            flops=2 * rows * width * n,
            bytes_accessed=2 * (len(items) * rows * width + width * total + rows * n),
            transcendentals=0,
        ),
        compiler_params=params(),
        name="partial_products",
    )(*flat, *weights)


def wide(a):
    return a.astype(jnp.float32)


def summed_direct(parts):
    arrived = []
    for part, shift in zip(parts[1:], (1, -1, 2)):
        arrived.append(along_y(part, shift))
    total = wide(parts[0])
    for part in arrived:
        total = total + wide(part)
    return total.astype(jnp.bfloat16)


def step_one(parts):
    _, plus, minus, _, _ = parts
    from_minus = along_y(plus, 1)
    return from_minus, along_y(minus, -1)


def step_two(parts, first):
    half = BLOCK // 2
    _, _, _, plus, minus = parts
    from_minus, from_plus = first
    to_plus = (wide(plus) + wide(from_minus[:half])).astype(jnp.bfloat16)
    to_minus = (wide(minus) + wide(from_plus[half:])).astype(jnp.bfloat16)
    a = along_y(to_plus, 1)
    return a, along_y(to_minus, -1)


def summed(parts, first, second):
    half = BLOCK // 2
    own = parts[0]
    from_minus, from_plus = first
    low = wide(own[:half]) + wide(from_plus[:half]) + wide(second[0])
    high = wide(own[half:]) + wide(from_minus[half:]) + wide(second[1])
    return jnp.concatenate([low, high], axis=0).astype(jnp.bfloat16)


def adapters_for_peers(peer_indices, own_z):
    per, rank, n = own_z[0].shape

    def kernel(*refs):
        indices, sources, outs, sems = refs[: NX - 1], refs[NX - 1 : NX - 1 + ZL], refs[NX - 1 + ZL : -1], refs[-1]
        x = lax.axis_index("gx") % NX
        zl = lax.axis_index("gx") // NX
        for r in range(NX - 1):
            for b in range(NY):
                a = indices[r][b]
                owner = a // per
                rz = jnp.where(owner % NX == x, (owner // NX - zl + ZL) % ZL, 0)
                for k in range(ZL):

                    @pl.when(rz == k)
                    def _():
                        pltpu.make_async_copy(sources[k].at[a % per], outs[r].at[b], sems.at[r, b]).start()

        for r in range(NX - 1):
            for b in range(NY):
                pltpu.make_async_copy(sources[0].at[0], outs[r].at[b], sems.at[r, b]).wait()

    return pl.pallas_call(
        kernel,
        in_specs=[smem()] * (NX - 1) + [hbm()] * ZL,
        out_specs=[hbm()] * (NX - 1),
        out_shape=[jax.ShapeDtypeStruct((NY, rank, n), jnp.bfloat16)] * (NX - 1),
        scratch_shapes=[pltpu.SemaphoreType.DMA((NX - 1, NY))],
        compiler_params=params(),
        name="adapters_for_peers",
    )(*peer_indices, *own_z)


def pick_adapters(index, own_z, received, shrinks):
    per, rank, n = own_z[0].shape

    def kernel(index_ref, *refs):
        sources, got, terms = refs[:ZL], refs[ZL : ZL + NX - 1], refs[ZL + NX - 1 : ZL + NX - 1 + NY]
        outs, sems = refs[ZL + NX - 1 + NY : -1], refs[-1]
        x = lax.axis_index("gx") % NX
        zl = lax.axis_index("gx") // NX
        y = lax.axis_index("gy")
        for k in range(NY):
            pltpu.make_async_copy(terms[k], outs[k].at[:, n:], sems.at[NY + k]).start()
            b = (y + k) % NY
            a = index_ref[b]
            owner = a // per
            back = (x - owner % NX + NX) % NX
            rz = (owner // NX - zl + ZL) % ZL
            for j in range(ZL):

                @pl.when(jnp.logical_and(back == 0, rz == j))
                def _():
                    pltpu.make_async_copy(sources[j].at[a % per], outs[k].at[:, :n], sems.at[k]).start()

            for r in range(1, NX):

                @pl.when(back == r)
                def _():
                    pltpu.make_async_copy(got[r - 1].at[b], outs[k].at[:, :n], sems.at[k]).start()

        for k in range(NY):
            pltpu.make_async_copy(sources[0].at[0], outs[k].at[:, :n], sems.at[k]).wait()
            pltpu.make_async_copy(terms[k], outs[k].at[:, n:], sems.at[NY + k]).wait()

    return pl.pallas_call(
        kernel,
        in_specs=[smem()] + [hbm()] * (ZL + NX - 1 + NY),
        out_specs=[hbm()] * NY,
        out_shape=[jax.ShapeDtypeStruct((rank, n + shrinks[0].shape[1]), jnp.bfloat16)] * NY,
        scratch_shapes=[pltpu.SemaphoreType.DMA((2 * NY,))],
        compiler_params=params(),
        name="pick_adapters",
    )(index, *own_z, *received, *shrinks)


def finish(live, ups, places, pieces, before=()):
    rank = ups[0].shape[0]
    n = ups[0].shape[1] - TERMS * BLOCK
    flat = [a for parts in pieces for a in parts]

    def kernel(live_ref, *refs):
        refs = refs[len(before) :]
        up_refs, ins = refs[:NY], list(refs[NY : NY + len(flat)])
        out_hbm, up_ref, out_ref, sems = refs[NY + len(flat) :]
        y = lax.axis_index("gy")
        zl = lax.axis_index("gx") // NX
        c = lax.axis_index("gz") % NC
        total = jnp.zeros((rank, BLOCK), jnp.float32)
        for k in range(NY):
            for term in range(TERMS):
                total = total + wide(up_refs[k][:, n + term * BLOCK : n + (term + 1) * BLOCK])
            up_ref[(y - k + NY) % NY] = up_refs[k][:, :n]
        low = total.astype(jnp.bfloat16)
        mask = lax.broadcasted_iota(jnp.int32, (BLOCK, n), 0) < live_ref[y]
        copies = []
        for i, (place, parts) in enumerate(zip(places, pieces)):
            col = (zl + place[0] + (place[1] - place[0]) * c) % ZL
            refs_here = [ins.pop(0) for _ in parts]
            halves = [(refs_here[0], 0, FIRST)]
            halves.append((refs_here[-1], 0 if len(parts) == 2 else NX * FIRST, n // NX - FIRST))
            expand = lax.dot_general(
                low, up_ref[col], (((0,), (0,)), ((), ())), preferred_element_type=jnp.float32
            )
            blocks = [
                ref[:, base + x * size : base + (x + 1) * size] for x in range(NX) for ref, base, size in halves
            ]
            value = wide(jnp.concatenate(blocks, axis=1)) + 2.0 * expand
            out_ref[i] = jnp.where(mask, value, 0.0).astype(jnp.bfloat16)
            there = out_hbm.at[:, pl.ds(pl.multiple_of(col * n, 128), n)]
            copies.append(pltpu.make_async_copy(out_ref.at[i], there, sems.at[i]))
            copies[-1].start()
        for copy in copies:
            copy.wait()

    vmem = pl.BlockSpec(memory_space=pltpu.VMEM)
    return pl.pallas_call(
        kernel,
        in_specs=[smem()] + [hbm()] * len(before) + [vmem] * (NY + len(flat)),
        out_specs=hbm(),
        out_shape=jax.ShapeDtypeStruct((BLOCK, n * ZL), jnp.bfloat16),
        scratch_shapes=[
            pltpu.VMEM((NY, rank, n), jnp.bfloat16),
            pltpu.VMEM((len(pieces), BLOCK, n), jnp.bfloat16),
            pltpu.SemaphoreType.DMA((len(pieces),)),
        ],
        input_output_aliases={1: 0} if before else {},
        compiler_params=params(),
        name="finish",
    )(live, *before, *ups, *flat)


FIRST = 128


def layer(tokens, base_up_weight, adapter_down_weight, adapter_up_weight, block_adapter_index, request_rows):
    rows, _ = tokens.shape
    y = lax.axis_index("gy")
    c = lax.axis_index("gz") % NC

    near = send(tokens, lambda z, x, c: ((z + 1 - 2 * c) % NZ, x, c))
    weights = []
    for part in (base_up_weight[:, :FIRST], base_up_weight[:, FIRST:]):
        pieces = [part.T]
        for r in range(1, NX):
            pieces.append(along_x(pieces[0], -r))
        weights.append(pieces)
    n = NX * base_up_weight.shape[1]
    up_z = [lax.dynamic_slice_in_dim(adapter_up_weight, y * n, n, 2)]
    for r in range(1, ZL):
        up_z.append(send(up_z[0], lambda z, x, c, r=r: (within(z, -r), x, c)))
    other = swap_cores(near)
    half = lax.dynamic_slice_in_dim(near, c * (rows // NC), rows // NC, 0)
    far = send(half, lambda z, x, c: ((z + 1 - 2 * c) % NZ, x, c))
    far_other = swap_cores(far)

    a = partial_products([((near,), 0, 1), ((other,), 0, 1)], weights[:1], direct=True)
    sum_a = summed_direct(a)
    b = partial_products([((near,), 1, 2), ((far, far_other), 0, 2)], weights)
    b1 = step_one(b)
    d = partial_products([((other,), 1, 2), ((tokens,), 0, 2)], weights)
    b2 = step_two(b, b1)
    d1 = step_one(d)
    cut, rest = NX * FIRST, n - NX * FIRST
    sum_b = summed(b, b1, b2)
    d2 = step_two(d, d1)
    sum_d = summed(d, d1, d2)

    def to_near(z, x, c):
        return within(z, 2 * c - 1), x, c

    def to_other(z, x, c):
        return within(z, 1 - 2 * c), x, c

    near0 = send(sum_a[:, :cut], to_near)
    other0 = send(sum_a[:, cut:], to_other)
    far = send(sum_b[:, rest:], lambda z, x, c: (within(z, 2), x, c))
    near1 = send(sum_b[:, :rest], to_near)
    other1 = send(sum_d[:, :rest], to_other)
    own = sum_d[:, rest:]

    shrinks = shrink(tokens, adapter_down_weight, block_adapter_index)
    peer_indices = []
    for r in range(1, NX):
        peer_indices.append(along_x(block_adapter_index, -r))
    received = list(adapters_for_peers(peer_indices, up_z))
    for r in range(1, NX):
        received[r - 1] = along_x(received[r - 1], r)
    ups = list(pick_adapters(block_adapter_index, up_z, received, shrinks))
    for k in range(1, NY):
        ups[k] = along_y(ups[k], k)
    ready = finish(request_rows, ups, ((0, 0), (1, 3), (2, 2)), ((own,), (near0, near1), (far,)))
    return finish(request_rows, ups, ((3, 1),), ((other0, other1),), (ready,))


def solution(mesh):
    in_specs = (
        P("gx", "gy"),
        P("gy", ("gz", "gx")),
        P(None, None, "gy"),
        P("gx", None, "gz"),
        P("gx"),
        P("gx"),
    )
    out_specs = P(("gx", "gy"), "gz")
    return jax.shard_map(layer, mesh=mesh, in_specs=in_specs, out_specs=out_specs, check_vma=False)
```

```python
import jax
import jax.numpy as jnp
from jax import lax
from jax.experimental import pallas as pl
from jax.experimental.pallas import tpu as pltpu
from jax.sharding import PartitionSpec as P


BLOCK = 128
ZL, NX, NY, ZH, NC = 4, 4, 4, 2, 2
TERMS = 3
NZ = ZL * ZH
VMEM_LIMIT = 20 * 2**20


def device_perm(move):
    def place(z, x, c):
        return (z % ZL * NX + x) * ZH * NC + z // ZL * NC + c

    return [(place(z, x, c), place(*move(z, x, c))) for z in range(NZ) for x in range(NX) for c in range(NC)]


def send(a, move):
    return lax.ppermute(a, ("gx", "gz"), device_perm(move))


def within(z, shift):
    return z // ZL * ZL + (z + shift) % ZL


def along_x(a, shift):
    return lax.ppermute(a, "gx", [(z * NX + x, z * NX + (x + shift) % NX) for z in range(ZL) for x in range(NX)])


def along_y(a, shift):
    return lax.ppermute(a, "gy", [(y, (y + shift) % NY) for y in range(NY)])


def swap_cores(a):
    return send(a, lambda z, x, c: (z, x, 1 - c))


def nt_dot(a, b):
    return lax.dot_general(a, b, (((1,), (1,)), ((), ())), preferred_element_type=jnp.float32)


def hbm():
    return pl.BlockSpec(memory_space=pltpu.HBM)


def smem():
    return pl.BlockSpec(memory_space=pltpu.SMEM)


def params():
    return pltpu.CompilerParams(vmem_limit_bytes=VMEM_LIMIT)


def shrink(tokens, down, index):
    rank, width = down.shape[1:]

    def kernel(index_ref, tok_hbm, down_hbm, *refs):
        outs, (tok_ref, down_ref, out_ref, sems) = refs[:NY], refs[NY:]
        y = lax.axis_index("gy")
        loads = [pltpu.make_async_copy(tok_hbm, tok_ref, sems.at[0])]
        for b in range(NY):
            loads.append(pltpu.make_async_copy(down_hbm.at[index_ref[b]], down_ref.at[b], sems.at[1 + b]))
        for copy in loads:
            copy.start()
        for copy in loads:
            copy.wait()
        for b in range(NY):
            rest = nt_dot(down_ref[b], tok_ref[pl.ds(b * BLOCK, BLOCK), :])
            for term in range(TERMS):
                part = rest.astype(jnp.bfloat16)
                out_ref[b, :, term * BLOCK : (term + 1) * BLOCK] = part
                rest = rest - part.astype(jnp.float32)
        stores = [
            pltpu.make_async_copy(out_ref.at[(y + k) % NY], outs[k], sems.at[k]) for k in range(NY)
        ]
        for copy in stores:
            copy.start()
        for copy in stores:
            copy.wait()

    return pl.pallas_call(
        kernel,
        in_specs=[smem(), hbm(), hbm()],
        out_specs=[hbm()] * NY,
        out_shape=[jax.ShapeDtypeStruct((rank, TERMS * BLOCK), jnp.bfloat16)] * NY,
        scratch_shapes=[
            pltpu.VMEM(tokens.shape, jnp.bfloat16),
            pltpu.VMEM((NY, rank, width), jnp.bfloat16),
            pltpu.VMEM((NY, rank, TERMS * BLOCK), jnp.bfloat16),
            pltpu.SemaphoreType.DMA((1 + NY,)),
        ],
        compiler_params=params(),
        name="shrink",
    )(index, tokens, down)


def partial_products(items, weight_sets, direct=False):
    weights = [w for pieces in weight_sets for w in pieces]
    width = weights[0].shape[1]
    set_rows = [NX * pieces[0].shape[0] for pieces in weight_sets]
    total = sum(set_rows)
    rows = NY * BLOCK
    flat = [a for arrays, _, _ in items for a in arrays]
    spans, n = [], 0
    for _, lo, hi in items:
        spans.append((sum(set_rows[:lo]), sum(set_rows[lo:hi]), n))
        n += spans[-1][1]
    half = BLOCK // 2
    part = rows // 2

    def kernel(*refs):
        ins, w_in = refs[: len(flat)], refs[len(flat) : len(flat) + len(weights)]
        outs = refs[len(flat) + len(weights) : -6]
        t_ref, w_ref, o_ref, in_sems, w_sems, out_sems = refs[-6:]
        x = lax.axis_index("gx") % NX
        y = lax.axis_index("gy")
        c = lax.axis_index("gz") % NC
        w_copies, base = [], 0
        for i, w in enumerate(weights):
            nb = w.shape[0]
            at = pl.multiple_of(base + (x + i % NX) % NX * nb, 32)
            w_copies.append(pltpu.make_async_copy(w_in[i], w_ref.at[pl.ds(at, nb), :], w_sems.at[i // NX]))
            if i % NX == NX - 1:
                base += NX * nb
        t_copies, at = [], 0
        for i, (arrays, _, _) in enumerate(items):
            for j, array in enumerate(arrays):
                size = array.shape[0]
                start = (j if len(arrays) == 1 else (c + j) % NC) * size
                dst = t_ref.at[i, pl.ds(pl.multiple_of(start, BLOCK), size), :]
                t_copies.append(pltpu.make_async_copy(ins[at], dst, in_sems.at[i]))
                at += 1
        first = len(items[0][0])
        lo, hi = items[0][1] * NX, items[0][2] * NX
        for copy in t_copies[:first] + w_copies[lo:hi] + w_copies[:lo] + w_copies[hi:] + t_copies[first:]:
            copy.start()
        done, there = [], set()
        for i, (low, size, col) in enumerate(spans):
            for k in range(items[i][1], items[i][2]):
                if k not in there:
                    here = w_ref.at[pl.ds(sum(set_rows[:k]), set_rows[k]), :]
                    pltpu.make_async_copy(here, here, w_sems.at[k]).wait()
                    there.add(k)
            pltpu.make_async_copy(t_ref.at[i], t_ref.at[i], in_sems.at[i]).wait()
            lanes = pl.ds(col, size)

            def step(j, carry):
                mine = pl.ds(pl.multiple_of(j * part, part), part)
                o_ref[mine, lanes] = nt_dot(t_ref[i, mine, :], w_ref[pl.ds(low, size), :]).astype(jnp.bfloat16)
                return carry

            lax.fori_loop(0, rows // part, step, 0)

            def rows_of(shift, low, size):
                start = (y + shift) % NY * BLOCK + low
                return o_ref.at[pl.ds(pl.multiple_of(start, half), size), lanes]

            whole = [(rows_of(shift, 0, BLOCK), out.at[:, lanes]) for shift, out in zip((0, 1, 3, 2), outs)]
            pairs = whole if direct else [
                (rows_of(2, 0, half), outs[1].at[:half, lanes]),
                (rows_of(1, half, half), outs[1].at[half:, lanes]),
                (rows_of(3, 0, half), outs[2].at[:half, lanes]),
                (rows_of(2, half, half), outs[2].at[half:, lanes]),
                (rows_of(1, 0, half), outs[3].at[:, lanes]),
                (rows_of(3, half, half), outs[4].at[:, lanes]),
                (rows_of(0, 0, BLOCK), outs[0].at[:, lanes]),
            ]
            for k, (src, dst) in enumerate(pairs):
                done.append(pltpu.make_async_copy(src, dst, out_sems.at[i, k]))
                done[-1].start()
        for copy in done:
            copy.wait()

    def out(m):
        return jax.ShapeDtypeStruct((m, n), jnp.bfloat16)

    return pl.pallas_call(
        kernel,
        in_specs=[hbm()] * (len(flat) + len(weights)),
        out_specs=[hbm()] * (4 if direct else 5),
        out_shape=[out(BLOCK)] * 4 if direct else [out(BLOCK)] * 3 + [out(half)] * 2,
        scratch_shapes=[
            pltpu.VMEM((len(items), rows, width), jnp.bfloat16),
            pltpu.VMEM((total, width), jnp.bfloat16),
            pltpu.VMEM((rows, n), jnp.bfloat16),
            pltpu.SemaphoreType.DMA((len(items),)),
            pltpu.SemaphoreType.DMA((len(weight_sets),)),
            pltpu.SemaphoreType.DMA((len(items), 7)),
        ],
        cost_estimate=pl.CostEstimate(
            flops=2 * rows * width * n,
            bytes_accessed=2 * (len(items) * rows * width + width * total + rows * n),
            transcendentals=0,
        ),
        compiler_params=params(),
        name="partial_products",
    )(*flat, *weights)


def wide(a):
    return a.astype(jnp.float32)


def summed_direct(parts):
    arrived = []
    for part, shift in zip(parts[1:], (1, -1, 2)):
        arrived.append(along_y(part, shift))
    total = wide(parts[0])
    for part in arrived:
        total = total + wide(part)
    return total.astype(jnp.bfloat16)


def step_one(parts):
    _, plus, minus, _, _ = parts
    from_minus = along_y(plus, 1)
    return from_minus, along_y(minus, -1)


def step_two(parts, first):
    half = BLOCK // 2
    _, _, _, plus, minus = parts
    from_minus, from_plus = first
    to_plus = (wide(plus) + wide(from_minus[:half])).astype(jnp.bfloat16)
    to_minus = (wide(minus) + wide(from_plus[half:])).astype(jnp.bfloat16)
    a = along_y(to_plus, 1)
    return a, along_y(to_minus, -1)


def summed(parts, first, second):
    half = BLOCK // 2
    own = parts[0]
    from_minus, from_plus = first
    low = wide(own[:half]) + wide(from_plus[:half]) + wide(second[0])
    high = wide(own[half:]) + wide(from_minus[half:]) + wide(second[1])
    return jnp.concatenate([low, high], axis=0).astype(jnp.bfloat16)


def pick_adapters(index, catalogs, shrinks):
    per, rank, n = catalogs[0].shape[1:]

    def kernel(index_ref, *refs):
        sources, terms, outs, sems = refs[:NX], refs[NX : NX + NY], refs[NX + NY : NX + 2 * NY], refs[NX + 2 * NY]
        for b in range(NY):
            pltpu.make_async_copy(terms[b], outs[b].at[:, n:], sems.at[NY + b]).start()
        x = lax.axis_index("gx") % NX
        zl = lax.axis_index("gx") // NX
        y = lax.axis_index("gy")
        for b in range(NY):
            a = index_ref[(y + b) % NY]
            owner = a // per
            rx = (owner % NX - x + NX) % NX
            rz = (owner // NX - zl + ZL) % ZL
            for k in range(NX):

                @pl.when(rx == k)
                def _():
                    pltpu.make_async_copy(sources[k].at[rz, a % per], outs[b].at[:, :n], sems.at[b]).start()

        for b in range(NY):
            pltpu.make_async_copy(sources[0].at[0, 0], outs[b].at[:, :n], sems.at[b]).wait()
            pltpu.make_async_copy(terms[b], outs[b].at[:, n:], sems.at[NY + b]).wait()

    return pl.pallas_call(
        kernel,
        in_specs=[smem()] + [hbm()] * (NX + NY),
        out_specs=[hbm()] * NY,
        out_shape=[jax.ShapeDtypeStruct((rank, n + shrinks[0].shape[1]), jnp.bfloat16)] * NY,
        scratch_shapes=[pltpu.SemaphoreType.DMA((2 * NY,))],
        compiler_params=params(),
        name="pick_adapters",
    )(index, *catalogs, *shrinks)


def finish(live, ups, places, pieces, before=()):
    rank = ups[0].shape[0]
    n = ups[0].shape[1] - TERMS * BLOCK
    flat = [a for parts in pieces for a in parts]

    def kernel(live_ref, *refs):
        refs = refs[len(before) :]
        up_refs, ins = refs[:NY], list(refs[NY : NY + len(flat)])
        out_hbm, up_ref, out_ref, sems = refs[NY + len(flat) :]
        y = lax.axis_index("gy")
        zl = lax.axis_index("gx") // NX
        c = lax.axis_index("gz") % NC
        total = jnp.zeros((rank, BLOCK), jnp.float32)
        for k in range(NY):
            for term in range(TERMS):
                total = total + wide(up_refs[k][:, n + term * BLOCK : n + (term + 1) * BLOCK])
            up_ref[(y - k + NY) % NY] = up_refs[k][:, :n]
        low = total.astype(jnp.bfloat16)
        mask = lax.broadcasted_iota(jnp.int32, (BLOCK, n), 0) < live_ref[y]
        copies = []
        for i, (place, parts) in enumerate(zip(places, pieces)):
            col = (zl + place[0] + (place[1] - place[0]) * c) % ZL
            refs_here = [ins.pop(0) for _ in parts]
            halves = [(refs_here[0], 0, FIRST)]
            halves.append((refs_here[-1], 0 if len(parts) == 2 else NX * FIRST, n // NX - FIRST))
            expand = lax.dot_general(
                low, up_ref[col], (((0,), (0,)), ((), ())), preferred_element_type=jnp.float32
            )
            blocks = [
                ref[:, base + x * size : base + (x + 1) * size] for x in range(NX) for ref, base, size in halves
            ]
            value = wide(jnp.concatenate(blocks, axis=1)) + 2.0 * expand
            out_ref[i] = jnp.where(mask, value, 0.0).astype(jnp.bfloat16)
            there = out_hbm.at[:, pl.ds(pl.multiple_of(col * n, 128), n)]
            copies.append(pltpu.make_async_copy(out_ref.at[i], there, sems.at[i]))
            copies[-1].start()
        for copy in copies:
            copy.wait()

    vmem = pl.BlockSpec(memory_space=pltpu.VMEM)
    return pl.pallas_call(
        kernel,
        in_specs=[smem()] + [hbm()] * len(before) + [vmem] * (NY + len(flat)),
        out_specs=hbm(),
        out_shape=jax.ShapeDtypeStruct((BLOCK, n * ZL), jnp.bfloat16),
        scratch_shapes=[
            pltpu.VMEM((NY, rank, n), jnp.bfloat16),
            pltpu.VMEM((len(pieces), BLOCK, n), jnp.bfloat16),
            pltpu.SemaphoreType.DMA((len(pieces),)),
        ],
        input_output_aliases={1: 0} if before else {},
        compiler_params=params(),
        name="finish",
    )(live, *before, *ups, *flat)


FIRST = 128


def layer(tokens, base_up_weight, adapter_down_weight, adapter_up_weight, block_adapter_index, request_rows):
    rows, _ = tokens.shape
    y = lax.axis_index("gy")
    c = lax.axis_index("gz") % NC

    near = send(tokens, lambda z, x, c: ((z + 1 - 2 * c) % NZ, x, c))
    weights = []
    for part in (base_up_weight[:, :FIRST], base_up_weight[:, FIRST:]):
        pieces = [part.T]
        for r in range(1, NX):
            pieces.append(along_x(pieces[0], -r))
        weights.append(pieces)
    n = NX * base_up_weight.shape[1]
    up_z = [lax.dynamic_slice_in_dim(adapter_up_weight, y * n, n, 2)]
    for r in range(1, ZL):
        up_z.append(send(up_z[0], lambda z, x, c, r=r: (within(z, -r), x, c)))
    other = swap_cores(near)
    half = lax.dynamic_slice_in_dim(near, c * (rows // NC), rows // NC, 0)
    far = send(half, lambda z, x, c: ((z + 1 - 2 * c) % NZ, x, c))
    far_other = swap_cores(far)

    a = partial_products([((near,), 0, 1), ((other,), 0, 1)], weights[:1], direct=True)
    sum_a = summed_direct(a)
    b = partial_products([((near,), 1, 2), ((far, far_other), 0, 2)], weights)
    b1 = step_one(b)
    d = partial_products([((other,), 1, 2), ((tokens,), 0, 2)], weights)
    b2 = step_two(b, b1)
    d1 = step_one(d)
    cut, rest = NX * FIRST, n - NX * FIRST
    sum_b = summed(b, b1, b2)
    d2 = step_two(d, d1)
    sum_d = summed(d, d1, d2)

    def to_near(z, x, c):
        return within(z, 2 * c - 1), x, c

    def to_other(z, x, c):
        return within(z, 1 - 2 * c), x, c

    near0 = send(sum_a[:, :cut], to_near)
    other0 = send(sum_a[:, cut:], to_other)
    far = send(sum_b[:, rest:], lambda z, x, c: (within(z, 2), x, c))
    near1 = send(sum_b[:, :rest], to_near)
    other1 = send(sum_d[:, :rest], to_other)
    own = sum_d[:, rest:]

    shrinks = shrink(tokens, adapter_down_weight, block_adapter_index)
    up_z = jnp.stack(up_z)
    catalogs = [up_z]
    for r in range(1, NX):
        catalogs.append(along_x(up_z, -r))
    ups = list(pick_adapters(block_adapter_index, catalogs, shrinks))
    for k in range(1, NY):
        ups[k] = along_y(ups[k], k)
    ready = finish(request_rows, ups, ((0, 0), (1, 3), (2, 2)), ((own,), (near0, near1), (far,)))
    return finish(request_rows, ups, ((3, 1),), ((other0, other1),), (ready,))


def solution(mesh):
    in_specs = (
        P("gx", "gy"),
        P("gy", ("gz", "gx")),
        P(None, None, "gy"),
        P("gx", None, "gz"),
        P("gx"),
        P("gx"),
    )
    out_specs = P(("gx", "gy"), "gz")
    return jax.shard_map(layer, mesh=mesh, in_specs=in_specs, out_specs=out_specs, check_vma=False)
```
